256 devices in a mesh: row: 16 (over y, x), col: 16 (over z, core).
Axes of the slice: x: 4, y: 4, z: 8, core: 2. Of those that a mesh axis runs over, the one named last changes fastest.
Arguments:
- trail: float32 [2, 16, 512, 2, 16, 512], P(None, 'row', None, None, 'col'), may hold values from -6 to 6
- panel: float32 [2, 16, 512, 512], P(None, 'row', None, 'col'), may hold values from -6 to 6
- row_basis: float32 [2, 16, 64, 512], P(None, 'row', None, 'col'), may hold values from -0.75 to 0.75
- row_coeff: float32 [2, 16, 64, 512], P(None, 'row', None, 'col'), may hold values from -0.25 to 0.25
- col_basis: float32 [2, 16, 64, 512], P(None, 'col', None, 'row'), may hold values from -0.75 to 0.75
- col_scaled: float32 [2, 16, 64, 512], P(None, 'col', None, 'row'), may hold values from -0.25 to 0.25
- pivot_basis: float32 [64, 512], P(None, 'col'), may hold values from -0.75 to 0.75
- pivot_scaled: float32 [64, 512], replicated, may hold values from -0.25 to 0.25
- sketch: float32 [64, 512], replicated, may hold values from -6 to 6
- perm: int32 [512], replicated, may hold values from 0 to 511, each once
- pair_kind: int32 [256], replicated, may hold values from 0 to 1
- pivot_values: float32 [3, 256], replicated, may hold values from -3 to 3, as said below
Outputs:
- trail_out: float32 [2, 16, 512, 2, 16, 512], P(None, 'row', None, None, 'col')
- basis_out: float32 [2, 16, 64, 512], P(None, 'row')
- coeff_out: float32 [2, 16, 64, 512], P(None, 'row')
The draws below stay inside these ranges and needn't reach their ends.
Inputs may be any that keep to these rules, and one draw needn't show every extreme that they name: `pivot_values`: rows 0 and 1 have magnitudes between 0.5 and 0.7; row 2 has magnitude 1.2 or more.
All inputs are finite; a program needn't handle non-finite values.
Results may differ from the reference program's by a relative error of at most 0.00013.
Values sent between devices are 32-bit elements; how exact they have to be, the bound alone decides.
A program may use at most 64 MiB of HBM per device.

```python
import jax
import jax.numpy as jnp
from jax import lax

B = 512
R = 64
LR = 2
LC = 2
PAIRS = 256
N_ROW = 16
N_COL = 16


def draw_pivot_values(key, part):
    first_key, second_key, third_key = jax.random.split(jax.random.fold_in(key, 17), 3)
    lowest, highest = (1.2, 2.0)
    magnitudes = jax.random.uniform(first_key, (2, PAIRS), jnp.float32, 0.5, 0.7)
    signs = jnp.where(jax.random.bernoulli(second_key, 0.5, (3, PAIRS)), 1.0, -1.0)
    offdiag = jax.random.uniform(third_key, (1, PAIRS), jnp.float32, lowest, highest)
    return jnp.concatenate([magnitudes, offdiag], axis=0) * signs


def place_ends(entries, stream_key, smallest, largest):
    place = [jax.random.randint(jax.random.fold_in(stream_key, axis), (), 0, length) for axis, length in enumerate(entries.shape)]
    main_axis = entries.shape.index(max(entries.shape))
    neighbour = place[:main_axis] + [(place[main_axis] + 1) % entries.shape[main_axis]] + place[main_axis + 1:]
    return entries.at[tuple(place)].set(smallest).at[tuple(neighbour)].set(largest)


def shard_levels(rng, dims, shards, smallest, high):
    loudness, own = 1.0, jax.random.fold_in(rng, 6)
    for position, blocks in shards:
        draws = jnp.exp(jax.random.uniform(jax.random.fold_in(own, position), (blocks,), jnp.float32, smallest / len(shards), high / len(shards)))
        loudness = loudness * jnp.repeat(draws, dims[position] // blocks).reshape([-1 if axis == position else 1 for axis in range(len(dims))])
    return loudness


def scatter_about(stream_key, shape, width, reach, shards=(), dtype=jnp.bfloat16):
    array = width * jax.random.normal(stream_key, shape, jnp.float32)
    if shards:
        array = array * shard_levels(stream_key, shape, shards, -0.22, 0.18)
    return jnp.clip(array, -reach, reach).astype(dtype)


def setup_inputs(seed: int = 0) -> dict:
    keys = jax.random.split(jax.random.key(seed), 13)
    trail = scatter_about(keys[0], (LR, N_ROW, B, LC, N_COL, B), 1.0, 6.0, ((1, 16), (4, 16)), jnp.float32)
    panel = scatter_about(keys[1], (LR, N_ROW, B, B), 1.0, 6.0, ((1, 16), (3, 16)), jnp.float32)
    row_basis = scatter_about(keys[2], (LR, N_ROW, R, B), R ** -0.5, 0.75, ((1, 16), (3, 16)), jnp.float32)
    row_coeff = scatter_about(keys[3], (LR, N_ROW, R, B), B ** -0.5, 0.25, ((1, 16), (3, 16)), jnp.float32)
    col_basis = scatter_about(keys[4], (LC, N_COL, R, B), R ** -0.5, 0.75, ((1, 16), (3, 16)), jnp.float32)
    col_scaled = scatter_about(keys[5], (LC, N_COL, R, B), B ** -0.5, 0.25, ((1, 16), (3, 16)), jnp.float32)
    pivot_basis = scatter_about(keys[6], (R, B), R ** -0.5, 0.75, ((1, 16),), jnp.float32)
    pivot_scaled = scatter_about(keys[7], (R, B), B ** -0.5, 0.25, (), jnp.float32)
    sketch = scatter_about(keys[8], (R, B), 1.0, 6.0, (), jnp.float32)
    perm = jax.random.permutation(keys[9], B).astype(jnp.int32)
    pair_kind = place_ends(jax.random.randint(keys[10], (PAIRS,), 0, 2), jax.random.fold_in(keys[10], 1), 0, 1).astype(jnp.int32)
    pivot_values = draw_pivot_values(jax.random.fold_in(keys[12], 71), 0)
    return {"trail": trail, "panel": panel, "row_basis": row_basis, "row_coeff": row_coeff, "col_basis": col_basis, "col_scaled": col_scaled, "pivot_basis": pivot_basis, "pivot_scaled": pivot_scaled, "sketch": sketch, "perm": perm, "pair_kind": pair_kind, "pivot_values": pivot_values}


def pair_apply(rows, pair_kind, pivot_values):
    shaped = rows.reshape(rows.shape[:-1] + (rows.shape[-1] // 2, 2))
    first_in = shaped[..., 0]
    second_in = shaped[..., 1]
    diag_one = pivot_values[0]
    diag_two = pivot_values[1]
    offdiag = pivot_values[2]
    determinant = diag_one * diag_two - offdiag * offdiag
    twin = pair_kind == 1
    first = jnp.where(twin, (first_in * diag_two - second_in * offdiag) / determinant, first_in / diag_one)
    second = jnp.where(twin, (second_in * diag_one - first_in * offdiag) / determinant, second_in / diag_two)
    return jnp.stack([first, second], axis=-1).reshape(rows.shape)

def reference(trail, panel, row_basis, row_coeff, col_basis, col_scaled, pivot_basis, pivot_scaled, sketch, perm, pair_kind, pivot_values):
    highest = lax.Precision.HIGHEST
    xrows = row_basis.reshape(LR * N_ROW, R, B)
    yrows = row_coeff.reshape(LR * N_ROW, R, B)
    zcols = col_basis.reshape(LC * N_COL, R, B)
    gcols = col_scaled.reshape(LC * N_COL, R, B)
    tiles = trail.reshape(LR * N_ROW, B, LC * N_COL, B)

    def one_row(item):
        tile, xrow, yrow = item
        core = jnp.einsum('rp,jsp->rjs', yrow, gcols, precision=highest)
        left = jnp.einsum('rp,rjs->pjs', xrow, core, precision=highest)
        change = jnp.einsum('pjs,jsq->pjq', left, zcols, precision=highest)
        return tile - change
    trail_out = lax.map(one_row, (tiles, xrows, yrows)).reshape(trail.shape)
    panels = panel.reshape(LR * N_ROW, B, B)
    pcore = jnp.einsum('irp,sp->irs', yrows, pivot_scaled, precision=highest)
    pleft = jnp.einsum('irp,irs->ips', xrows, pcore, precision=highest)
    updated = panels - jnp.einsum('ips,sq->ipq', pleft, pivot_basis, precision=highest)
    scaled_t = pair_apply(sketch, pair_kind, pivot_values)
    permuted = jnp.take(updated, perm, axis=2)
    range_t = jnp.einsum('ipt,rt->irp', permuted, scaled_t, precision=highest)
    gram = jnp.einsum('irp,isp->irs', range_t, range_t, precision=highest) / B
    lower = jnp.linalg.cholesky(gram)
    basis = jax.vmap(lambda low, rhs: jax.scipy.linalg.solve_triangular(low, rhs, lower=True))(lower, range_t)
    projected = jnp.einsum('irp,ipt->irt', basis, permuted, precision=highest)
    coeff = pair_apply(projected, pair_kind, pivot_values) / jnp.sqrt(jnp.float32(B))
    return (trail_out, basis.reshape(LR, N_ROW, R, B), coeff.reshape(LR, N_ROW, R, B))
```

```python
import functools

import jax
import jax.numpy as jnp
from jax import lax
from jax.experimental import pallas as pl
from jax.experimental.pallas import tpu as pltpu
from jax.sharding import PartitionSpec as P

MESH = pl.DeviceIdType.MESH
F32 = jnp.float32
BF16 = jnp.bfloat16
HIGHEST = lax.Precision.HIGHEST
NN = (((1,), (0,)), ((), ()))
NT = (((1,), (1,)), ((), ()))
TN = (((0,), (0,)), ((), ()))
VMEM = pl.BlockSpec(memory_space=pltpu.VMEM)


def dot(a, b, dims=NN):
    return lax.dot_general(a, b, dims, precision=HIGHEST, preferred_element_type=F32)


def split3(x):
    high = x.astype(BF16)
    rest = x - high.astype(F32)
    mid = rest.astype(BF16)
    low = (rest - mid.astype(F32)).astype(BF16)
    return jnp.concatenate([high, mid, low], axis=0)


def select_dot(x, chosen, dims):
    n = x.shape[0]
    out = lax.dot_general(split3(x), chosen, dims, preferred_element_type=F32)
    return (out[2 * n :] + out[n : 2 * n]) + out[:n]


def lower_half(shape):
    return lax.broadcasted_iota(jnp.int32, shape, 1) % 128 < 64


def swap(x):
    return pltpu.roll(x, 64, 1)


def fold(x):
    return jnp.where(lower_half((32, 128)), x[:32], swap(x[32:]))


def unfold(ref):
    low = lower_half((32, 128))
    tops, bottoms = [], []
    for j in range(4):
        even, odd = ref[2 * j], ref[2 * j + 1]
        tops.append(jnp.where(low, even, swap(odd)))
        bottoms.append(jnp.where(low, swap(even), odd))
    return jnp.concatenate([jnp.concatenate(tops, axis=1), jnp.concatenate(bottoms, axis=1)], axis=0)


def inverse_factor(gram):
    rows = lax.broadcasted_iota(jnp.int32, (64, 64), 0)
    eye = (rows == lax.broadcasted_iota(jnp.int32, (64, 64), 1)).astype(F32)
    both = jnp.concatenate([gram, eye], axis=1)
    work = [both[8 * g : 8 * g + 8] for g in range(8)]
    sub = lax.broadcasted_iota(jnp.int32, (8, 128), 0)
    for k in range(8):
        columns = {
            (g, j): jnp.broadcast_to(work[g][:, 8 * k + j : 8 * k + j + 1], (8, 128))
            for g in range(k, 8)
            for j in range(8)
        }
        pivots = jnp.ones((8, 128), F32)
        for j in range(8):
            pivot = jnp.broadcast_to(columns[k, j][j : j + 1], (8, 128))
            pivots = jnp.where(sub == j, pivot, pivots)
            inverse = 1.0 / pivot
            scaled = jnp.broadcast_to(work[k][j : j + 1], (8, 128)) * inverse
            heads = {
                later: jnp.broadcast_to(columns[k, later][j : j + 1], (8, 128)) * inverse
                for later in range(j + 1, 8)
            }
            for g in range(k, 8):
                factor = columns[g, j]
                if g == k:
                    if j == 7:
                        continue
                    factor = jnp.where(sub > j, factor, 0.0)
                work[g] = work[g] - factor * scaled
                for later in range(j + 1, 8):
                    columns[g, later] = columns[g, later] - factor * heads[later]
        work[k] = work[k] * lax.rsqrt(pivots)
    return jnp.concatenate(work, axis=0)


def panel_kernel(
    n_row,
    panel,
    row_basis,
    row_coeff,
    col_basis,
    col_scaled,
    pivot_basis,
    pivot_scaled,
    sketch,
    perm,
    pair_kind,
    pivot_values,
    xy,
    zg,
    ranges,
    coeffs,
    inverses,
    pan_send,
    pan_recv,
    pan_chip,
    pan_full,
    xy_send,
    zg_send,
    rng_send,
    rng_recv,
    c_send,
    c_recv,
    basis_full,
    chosen,
    updated,
    pan_ss,
    pan_rs,
    xy_ss,
    xy_rs,
    zg_ss,
    zg_rs,
    rng_ss,
    rng_rs,
    c_ss,
    c_rs,
    peer_ss,
    peer_rs,
):
    r = lax.axis_index("row")
    c = lax.axis_index("col")
    z = c // 2
    k = c % 2
    peer = 2 * z + 1 - k

    barrier = pltpu.get_barrier_semaphore()
    for d in range(1, 16):
        pl.semaphore_signal(barrier, inc=1, device_id=(r, (c + d) % 16), device_id_type=MESH)
    for d in range(1, n_row):
        pl.semaphore_signal(barrier, inc=1, device_id=((r + d) % n_row, c), device_id_type=MESH)

    low16 = lower_half((16, 128))
    for a in range(2):
        for j in range(4):
            tile = panel[a, :, 128 * j : 128 * j + 128]
            top, bottom = tile[:16], tile[16:]
            pan_send[a, 2 * j] = jnp.where(low16, top, swap(bottom))
            pan_send[a, 2 * j + 1] = jnp.where(low16, swap(top), bottom)
        xy_send[a, :32, :64] = row_basis[a]
        xy_send[a, :32, 64:] = row_coeff[a]
        xy_send[a, 32:, :64] = pivot_basis[16 * a : 16 * a + 8]
        xy_send[a, 32:, 64:] = pivot_basis[16 * a + 8 : 16 * a + 16]
        zg_send[a, :, :64] = col_basis[a]
        zg_send[a, :, 64:] = col_scaled[a]
    pan_recv[c] = pan_send[k, z]
    xy[k, c] = xy_send[k]
    zg[r] = zg_send[...]
    pan_chip[k] = panel[k]

    pl.semaphore_wait(barrier, 14 + n_row)

    def copy(src, dst, send_sem, recv_sem, row, col):
        return pltpu.make_async_remote_copy(
            src_ref=src,
            dst_ref=dst,
            send_sem=send_sem,
            recv_sem=recv_sem,
            device_id=(row, col),
            device_id_type=MESH,
        )

    sends = []

    def send(*args):
        one = copy(*args)
        one.start()
        sends.append(one)

    def to_peer(i, src, dst):
        send(src, dst, peer_ss.at[i], peer_rs.at[i], r, peer)

    def from_peer(i, ref):
        copy(ref, ref, peer_ss.at[i], peer_rs.at[i], r, peer).wait_recv()

    order = [8, 9, 7, 10, 6, 11, 5, 12, 4, 13, 3, 14, 2, 15, 1]
    for d in order:
        to = (c + d) % 16
        send(pan_send.at[to % 2, to // 2], pan_recv.at[c], pan_ss.at[d], pan_rs.at[c], r, to)
    to_peer(0, panel.at[1 - k], pan_chip.at[k])
    for d in order:
        to = (c + d) % 16
        send(xy_send.at[to % 2], xy.at[to % 2, c], xy_ss.at[d], xy_rs.at[c], r, to)
    for d in range(1, n_row):
        to = (r + d) % n_row
        send(zg_send, zg.at[r], zg_ss.at[d], zg_rs.at[r], to, c)

    q_ids = lax.broadcasted_iota(jnp.int32, (512, 512), 0)
    chosen[...] = (q_ids == perm[...]).astype(F32).astype(BF16)
    t_ids = lax.broadcasted_iota(jnp.int32, (256, 512), 1)
    spread = (t_ids // 2 == lax.broadcasted_iota(jnp.int32, (256, 512), 0)).astype(F32).astype(BF16)
    values = jnp.concatenate([pivot_values[...], pair_kind[...].astype(F32), jnp.zeros((4, 256), F32)], axis=0)
    values = select_dot(values, spread, NN)
    first, second, offdiag, twin = values[0:1], values[1:2], values[2:3], values[3:4] > 0.5
    odd = lax.broadcasted_iota(jnp.int32, (1, 512), 1) % 2 == 1
    own = jnp.where(odd, second, first)
    other = jnp.where(odd, first, second)
    determinant = first * second - offdiag * offdiag
    alpha = jnp.where(twin, other / determinant, 1.0 / own)
    beta = jnp.where(twin, -offdiag / determinant, 0.0)

    def pair_apply(x):
        partner = jnp.where(odd, pltpu.roll(x, 1, 1), pltpu.roll(x, 511, 1))
        return x * alpha + partner * beta

    scaled = select_dot(pair_apply(sketch[...]), chosen[...], NT)

    for d in order:
        at = (c + d) % 16
        copy(pan_recv.at[at], pan_recv.at[at], pan_ss.at[0], pan_rs.at[at], r, at).wait_recv()
    for i in range(16):
        block = pan_recv[i]
        pan_full[32 * i : 32 * i + 16] = block
        pan_full[32 * i + 16 : 32 * i + 32] = swap(block)
    folded = fold(dot(scaled, pan_full[...]))
    rng_send[...] = folded
    rng_recv[z] = folded
    steps = [4, 5, 3, 6, 2, 7, 1]
    for d in steps:
        to = 2 * ((z + d) % 8) + k
        send(rng_send, rng_recv.at[z], rng_ss.at[d], rng_rs.at[z], r, to)

    for d in order:
        at = (c + d) % 16
        copy(xy.at[k, at], xy.at[k, at], xy_ss.at[0], xy_rs.at[at], r, at).wait_recv()
    to_peer(1, xy.at[k], xy.at[k])
    pivot_core = jnp.zeros((64, 128), F32)
    left = xy[k, :, :32].reshape(512, 128)
    pivot_core = dot(pivot_scaled[...], left)
    from_peer(0, pan_chip.at[1 - k])
    from_peer(1, xy.at[1 - k])
    for i in range(16):
        for half in range(2):
            block = xy[half, i, 32:]
            at = 32 * i + 16 * half
            basis_full[at : at + 8] = block
            basis_full[at + 8 : at + 16] = swap(block)
    weights = dot(scaled, basis_full[...])[:, :64]
    mine = basis_full[pl.ds(pl.multiple_of(64 * z, 64), 64), :][:, :64]
    mixed = dot(jnp.concatenate([weights, mine], axis=0), pivot_core)
    mixed = jnp.where(lower_half((128, 128)), swap(mixed), 0.0)
    fixes = dot(mixed, left, NT)
    updated[64:] = pan_chip[...].reshape(64, 512) - fixes[64:]

    for d in steps:
        at = (z + d) % 8
        copy(rng_recv.at[at], rng_recv.at[at], rng_ss.at[0], rng_rs.at[at], r, 2 * at + k).wait_recv()
    total = unfold(rng_recv) - fixes[:64]
    updated[:64] = total
    ranges[k] = total
    products = dot(total, updated[...], NT)
    folded = fold(swap(products))
    c_send[...] = folded
    c_recv[z] = folded
    for d in steps:
        to = 2 * ((z + d) % 8) + k
        send(c_send, c_recv.at[z], c_ss.at[d], c_rs.at[z], r, to)
    to_peer(2, ranges.at[k], ranges.at[k])

    inverses[k] = swap(inverse_factor(products[:, :64] * (1.0 / 512.0)))
    to_peer(3, inverses.at[k], inverses.at[k])

    for d in steps:
        at = (z + d) % 8
        copy(c_recv.at[at], c_recv.at[at], c_ss.at[0], c_rs.at[at], r, 2 * at + k).wait_recv()
    permuted = select_dot(unfold(c_recv), chosen[...], NN)
    coeffs[k] = pair_apply(permuted) * (512.0**-0.5)
    to_peer(4, coeffs.at[k], coeffs.at[k])

    for d in range(1, n_row):
        at = (r + d) % n_row
        copy(zg.at[at], zg.at[at], zg_ss.at[0], zg_rs.at[at], at, c).wait_recv()
    from_peer(2, ranges.at[1 - k])
    from_peer(3, inverses.at[1 - k])
    from_peer(4, coeffs.at[1 - k])
    for one in sends:
        one.wait_send()


def trail_kernel(xy, zg, ranges, coeffs, inverses, trail, trail_out, basis_out, coeff_out, lefts, rights):
    step = pl.program_id(0)

    @pl.when(step == 0)
    def _():
        low = lower_half((512, 128))
        for b in range(2):
            both = zg[:, b].reshape(512, 128)
            twice = jnp.where(low, both, swap(both))
            high = twice.astype(BF16).astype(F32)
            pair = jnp.where(low, high, twice - high).astype(BF16)
            rights[b] = jnp.concatenate([pair, pair], axis=1)
        for a in range(2):
            rows = xy[a, :, :32].reshape(512, 128)
            for b in range(2):
                both = zg[:, b].reshape(512, 128)
                core = dot(rows, both, TN)[64:, 64:]
                core = jnp.concatenate([core, core], axis=1)
                core = jnp.concatenate([core, jnp.zeros((64, 128), F32)], axis=0)
                left = dot(rows, core)
                high = left.astype(BF16)
                lefts[a, b] = jnp.concatenate([high, (left - high.astype(F32)).astype(BF16)], axis=1)
            inverse = inverses[a][:, :64]
            basis_out[a] = dot(inverse, ranges[a])
            coeff_out[a] = dot(inverse, coeffs[a])

    a = step // 4
    at = pl.multiple_of((step % 4) * 128, 128)
    for b in range(2):
        change = lax.dot_general(
            lefts[a, b, pl.ds(at, 128), :], rights[b], NT, preferred_element_type=F32
        )
        for j in range(4):
            rows = pl.ds(4 * b + j, 128, stride=8)
            trail_out[rows, :] = trail[rows, :] - change[:, 128 * j : 128 * j + 128]


def body(n_row, trail, panel, row_basis, row_coeff, col_basis, col_scaled, pivot_basis, pivot_scaled, sketch, perm, pair_kind, pivot_values):
    turn = lambda x: jnp.swapaxes(x[:, 0], 1, 2)
    dma = pltpu.SemaphoreType.DMA
    xy, zg, ranges, coeffs, inverses = pl.pallas_call(
        functools.partial(panel_kernel, n_row),
        out_shape=(
            jax.ShapeDtypeStruct((2, 16, 40, 128), F32),
            jax.ShapeDtypeStruct((n_row, 2, 32, 128), F32),
            jax.ShapeDtypeStruct((2, 64, 512), F32),
            jax.ShapeDtypeStruct((2, 64, 512), F32),
            jax.ShapeDtypeStruct((2, 64, 128), F32),
        ),
        in_specs=[VMEM] * 11,
        out_specs=(VMEM,) * 5,
        scratch_shapes=[
            pltpu.VMEM((2, 8, 16, 128), F32),
            pltpu.VMEM((16, 16, 128), F32),
            pltpu.VMEM((2, 32, 512), F32),
            pltpu.VMEM((512, 128), F32),
            pltpu.VMEM((2, 40, 128), F32),
            pltpu.VMEM((2, 32, 128), F32),
            pltpu.VMEM((32, 128), F32),
            pltpu.VMEM((8, 32, 128), F32),
            pltpu.VMEM((32, 128), F32),
            pltpu.VMEM((8, 32, 128), F32),
            pltpu.VMEM((512, 128), F32),
            pltpu.VMEM((512, 512), BF16),
            pltpu.VMEM((128, 512), F32),
            dma((16,)),
            dma((16,)),
            dma((16,)),
            dma((16,)),
            dma((n_row,)),
            dma((n_row,)),
            dma((8,)),
            dma((8,)),
            dma((8,)),
            dma((8,)),
            dma((5,)),
            dma((5,)),
        ],
        compiler_params=pltpu.CompilerParams(
            collective_id=0, has_side_effects=True, vmem_limit_bytes=24 * 1024 * 1024
        ),
        name="panel",
    )(
        turn(panel),
        turn(row_basis),
        turn(row_coeff),
        turn(col_basis),
        turn(col_scaled),
        pivot_basis.T,
        pivot_scaled,
        sketch,
        perm.reshape(1, 512),
        pair_kind.reshape(1, 256),
        pivot_values,
    )
    block = pl.BlockSpec((1024, 128), lambda i: (i, 0))
    trail_out, basis_out, coeff_out = pl.pallas_call(
        trail_kernel,
        grid=(8,),
        out_shape=(
            jax.ShapeDtypeStruct((8192, 128), F32),
            jax.ShapeDtypeStruct((2, 64, 512), F32),
            jax.ShapeDtypeStruct((2, 64, 512), F32),
        ),
        in_specs=[VMEM] * 5 + [block],
        out_specs=(block, VMEM, VMEM),
        scratch_shapes=[pltpu.VMEM((2, 2, 512, 256), BF16), pltpu.VMEM((2, 512, 256), BF16)],
        compiler_params=pltpu.CompilerParams(vmem_limit_bytes=24 * 1024 * 1024),
        name="trail",
    )(xy, zg, ranges, coeffs, inverses, trail.reshape(8192, 128))
    return (trail_out.reshape(trail.shape), basis_out[:, None], coeff_out[:, None])


def solution(mesh):
    n_row = mesh.shape["row"]
    return jax.shard_map(
        functools.partial(body, n_row),
        mesh=mesh,
        in_specs=(
            P(None, "row", None, None, "col", None),
            P(None, "row", None, "col"),
            P(None, "row", None, "col"),
            P(None, "row", None, "col"),
            P(None, "col", None, "row"),
            P(None, "col", None, "row"),
            P(None, "col"),
            P(),
            P(),
            P(),
            P(),
            P(),
        ),
        out_specs=(
            P(None, "row", None, None, "col", None),
            P(None, "row", None, None),
            P(None, "row", None, None),
        ),
        check_vma=False,
    )
```

```python
import functools

import jax
import jax.numpy as jnp
from jax import lax
from jax.experimental import pallas as pl
from jax.experimental.pallas import tpu as pltpu
from jax.sharding import PartitionSpec as P

MESH = pl.DeviceIdType.MESH
F32 = jnp.float32
BF16 = jnp.bfloat16
HIGHEST = lax.Precision.HIGHEST
NN = (((1,), (0,)), ((), ()))
NT = (((1,), (1,)), ((), ()))
TN = (((0,), (0,)), ((), ()))
VMEM = pl.BlockSpec(memory_space=pltpu.VMEM)
HBM = pl.BlockSpec(memory_space=pltpu.HBM)


def dot(a, b, dims=NN):
    return lax.dot_general(a, b, dims, precision=HIGHEST, preferred_element_type=F32)


def split3(x):
    high = x.astype(BF16)
    rest = x - high.astype(F32)
    mid = rest.astype(BF16)
    low = (rest - mid.astype(F32)).astype(BF16)
    return jnp.concatenate([high, mid, low], axis=0)


def select_dot(x, chosen, dims):
    n = x.shape[0]
    out = lax.dot_general(split3(x), chosen, dims, preferred_element_type=F32)
    return (out[2 * n :] + out[n : 2 * n]) + out[:n]


def lower_half(shape):
    return lax.broadcasted_iota(jnp.int32, shape, 1) % 128 < 64


def swap(x):
    return pltpu.roll(x, 64, 1)


def fold(x):
    return jnp.where(lower_half((32, 128)), x[:32], swap(x[32:]))


def unfold(ref):
    low = lower_half((32, 128))
    tops, bottoms = [], []
    for j in range(4):
        even, odd = ref[2 * j], ref[2 * j + 1]
        tops.append(jnp.where(low, even, swap(odd)))
        bottoms.append(jnp.where(low, swap(even), odd))
    return jnp.concatenate([jnp.concatenate(tops, axis=1), jnp.concatenate(bottoms, axis=1)], axis=0)


def inverse_factor(gram):
    rows = lax.broadcasted_iota(jnp.int32, (64, 64), 0)
    eye = (rows == lax.broadcasted_iota(jnp.int32, (64, 64), 1)).astype(F32)
    both = jnp.concatenate([gram, eye], axis=1)
    work = [both[8 * g : 8 * g + 8] for g in range(8)]
    sub = lax.broadcasted_iota(jnp.int32, (8, 128), 0)
    for k in range(8):
        columns = {
            (g, j): jnp.broadcast_to(work[g][:, 8 * k + j : 8 * k + j + 1], (8, 128))
            for g in range(k, 8)
            for j in range(8)
        }
        pivots = jnp.ones((8, 128), F32)
        for j in range(8):
            pivot = jnp.broadcast_to(columns[k, j][j : j + 1], (8, 128))
            pivots = jnp.where(sub == j, pivot, pivots)
            inverse = 1.0 / pivot
            scaled = jnp.broadcast_to(work[k][j : j + 1], (8, 128)) * inverse
            heads = {
                later: jnp.broadcast_to(columns[k, later][j : j + 1], (8, 128)) * inverse
                for later in range(j + 1, 8)
            }
            for g in range(k, 8):
                factor = columns[g, j]
                if g == k:
                    if j == 7:
                        continue
                    factor = jnp.where(sub > j, factor, 0.0)
                work[g] = work[g] - factor * scaled
                for later in range(j + 1, 8):
                    columns[g, later] = columns[g, later] - factor * heads[later]
        work[k] = work[k] * lax.rsqrt(pivots)
    return jnp.concatenate(work, axis=0)


def panel_kernel(
    n_row,
    trail_hbm,
    *refs,
):
    inputs, refs = refs[:11], refs[11:]
    run_panel(n_row, trail_hbm, inputs, *refs)


def run_panel(
    n_row,
    trail_hbm,
    inputs,
    trail,
    ranges,
    coeffs,
    inverses,
    xy,
    zg,
    staged,
    pan_send,
    pan_recv,
    pan_chip,
    pan_full,
    xy_send,
    zg_send,
    rng_send,
    rng_recv,
    c_send,
    c_recv,
    basis_full,
    chosen,
    updated,
    pan_ss,
    pan_rs,
    xy_ss,
    xy_rs,
    zg_ss,
    zg_rs,
    rng_ss,
    rng_rs,
    c_ss,
    c_rs,
    peer_ss,
    peer_rs,
    in_sem,
    trail_sem,
    lefts,
    rights,
):
    r = lax.axis_index("row")
    c = lax.axis_index("col")
    z = c // 2
    k = c % 2
    peer = 2 * z + 1 - k

    loads = [pltpu.make_async_copy(src, dst, in_sem.at[i]) for i, (src, dst) in enumerate(zip(inputs, staged))]
    for one in loads:
        one.start()
    trail_load = pltpu.make_async_copy(trail_hbm, trail, trail_sem)
    panel, row_basis, row_coeff, pivot_basis, col_basis, col_scaled, sketch, perm, pair_kind, pivot_values, pivot_scaled = staged

    barrier = pltpu.get_barrier_semaphore()
    for d in range(1, 16):
        pl.semaphore_signal(barrier, inc=1, device_id=(r, (c + d) % 16), device_id_type=MESH)
    for d in range(1, n_row):
        pl.semaphore_signal(barrier, inc=1, device_id=((r + d) % n_row, c), device_id_type=MESH)

    for one in loads:
        one.wait()
    low16 = lower_half((16, 128))
    for a in range(2):
        for j in range(4):
            tile = panel[a, :, 128 * j : 128 * j + 128]
            top, bottom = tile[:16], tile[16:]
            pan_send[a, 2 * j] = jnp.where(low16, top, swap(bottom))
            pan_send[a, 2 * j + 1] = jnp.where(low16, swap(top), bottom)
        xy_send[a, :32, :64] = row_basis[a]
        xy_send[a, :32, 64:] = row_coeff[a]
        xy_send[a, 32:, :64] = pivot_basis[16 * a : 16 * a + 8]
        xy_send[a, 32:, 64:] = pivot_basis[16 * a + 8 : 16 * a + 16]
        zg_send[a, :, :64] = col_basis[a]
        zg_send[a, :, 64:] = col_scaled[a]
    pan_recv[c] = pan_send[k, z]
    xy[k, c] = xy_send[k]
    zg[r] = zg_send[...]
    pan_chip[k] = panel[k]

    pl.semaphore_wait(barrier, 14 + n_row)

    def copy(src, dst, send_sem, recv_sem, row, col):
        return pltpu.make_async_remote_copy(
            src_ref=src,
            dst_ref=dst,
            send_sem=send_sem,
            recv_sem=recv_sem,
            device_id=(row, col),
            device_id_type=MESH,
        )

    sends = []

    def send(*args):
        one = copy(*args)
        one.start()
        sends.append(one)

    def to_peer(i, src, dst):
        send(src, dst, peer_ss.at[i], peer_rs.at[i], r, peer)

    def from_peer(i, ref):
        copy(ref, ref, peer_ss.at[i], peer_rs.at[i], r, peer).wait_recv()

    order = [8, 9, 7, 10, 6, 11, 5, 12, 4, 13, 3, 14, 2, 15, 1]
    for d in order:
        to = (c + d) % 16
        send(pan_send.at[to % 2, to // 2], pan_recv.at[c], pan_ss.at[d], pan_rs.at[c], r, to)
    to_peer(0, panel.at[1 - k], pan_chip.at[k])
    for d in order:
        to = (c + d) % 16
        send(xy_send.at[to % 2], xy.at[to % 2, c], xy_ss.at[d], xy_rs.at[c], r, to)
    for d in range(1, n_row):
        to = (r + d) % n_row
        send(zg_send, zg.at[r], zg_ss.at[d], zg_rs.at[r], to, c)

    trail_load.start()
    q_ids = lax.broadcasted_iota(jnp.int32, (512, 512), 0)
    chosen[...] = (q_ids == perm[...]).astype(F32).astype(BF16)
    t_ids = lax.broadcasted_iota(jnp.int32, (256, 512), 1)
    spread = (t_ids // 2 == lax.broadcasted_iota(jnp.int32, (256, 512), 0)).astype(F32).astype(BF16)
    values = jnp.concatenate([pivot_values[...], pair_kind[...].astype(F32), jnp.zeros((4, 256), F32)], axis=0)
    values = select_dot(values, spread, NN)
    first, second, offdiag, twin = values[0:1], values[1:2], values[2:3], values[3:4] > 0.5
    odd = lax.broadcasted_iota(jnp.int32, (1, 512), 1) % 2 == 1
    own = jnp.where(odd, second, first)
    other = jnp.where(odd, first, second)
    determinant = first * second - offdiag * offdiag
    alpha = jnp.where(twin, other / determinant, 1.0 / own)
    beta = jnp.where(twin, -offdiag / determinant, 0.0)

    def pair_apply(x):
        partner = jnp.where(odd, pltpu.roll(x, 1, 1), pltpu.roll(x, 511, 1))
        return x * alpha + partner * beta

    scaled = select_dot(pair_apply(sketch[...]), chosen[...], NT)

    for d in order:
        at = (c + d) % 16
        copy(pan_recv.at[at], pan_recv.at[at], pan_ss.at[0], pan_rs.at[at], r, at).wait_recv()
    for i in range(16):
        block = pan_recv[i]
        pan_full[32 * i : 32 * i + 16] = block
        pan_full[32 * i + 16 : 32 * i + 32] = swap(block)
    folded = fold(dot(scaled, pan_full[...]))
    rng_send[...] = folded
    rng_recv[z] = folded
    steps = [4, 5, 3, 6, 2, 7, 1]
    for d in steps:
        to = 2 * ((z + d) % 8) + k
        send(rng_send, rng_recv.at[z], rng_ss.at[d], rng_rs.at[z], r, to)

    for d in order:
        at = (c + d) % 16
        copy(xy.at[k, at], xy.at[k, at], xy_ss.at[0], xy_rs.at[at], r, at).wait_recv()
    to_peer(1, xy.at[k], xy.at[k])
    left = xy[k, :, :32].reshape(512, 128)
    pivot_core = dot(pivot_scaled[...], left)
    from_peer(0, pan_chip.at[1 - k])
    from_peer(1, xy.at[1 - k])
    for i in range(16):
        for half in range(2):
            block = xy[half, i, 32:]
            at = 32 * i + 16 * half
            basis_full[at : at + 8] = block
            basis_full[at + 8 : at + 16] = swap(block)
    weights = dot(scaled, basis_full[...])[:, :64]
    mine = basis_full[pl.ds(pl.multiple_of(64 * z, 64), 64), :][:, :64]
    mixed = dot(jnp.concatenate([weights, mine], axis=0), pivot_core)
    mixed = jnp.where(lower_half((128, 128)), swap(mixed), 0.0)
    fixes = dot(mixed, left, NT)
    updated[64:] = pan_chip[...].reshape(64, 512) - fixes[64:]

    for d in steps:
        at = (z + d) % 8
        copy(rng_recv.at[at], rng_recv.at[at], rng_ss.at[0], rng_rs.at[at], r, 2 * at + k).wait_recv()
    total = unfold(rng_recv) - fixes[:64]
    updated[:64] = total
    ranges[k] = total
    products = dot(total, updated[...], NT)
    folded = fold(swap(products))
    c_send[...] = folded
    c_recv[z] = folded
    for d in steps:
        to = 2 * ((z + d) % 8) + k
        send(c_send, c_recv.at[z], c_ss.at[d], c_rs.at[z], r, to)
    to_peer(2, ranges.at[k], ranges.at[k])

    for d in range(1, n_row):
        at = (r + d) % n_row
        copy(zg.at[at], zg.at[at], zg_ss.at[0], zg_rs.at[at], at, c).wait_recv()
    trail_load.wait()
    inverses[k] = swap(inverse_factor(products[:, :64] * (1.0 / 512.0)))
    to_peer(3, inverses.at[k], inverses.at[k])
    low = lower_half((512, 128))
    columns = []
    for b in range(2):
        both = zg[:, b].reshape(512, 128)
        columns.append(both)
        twice = jnp.where(low, both, swap(both))
        high = twice.astype(BF16).astype(F32)
        pair = jnp.where(low, high, twice - high).astype(BF16)
        rights[b] = jnp.concatenate([pair, pair], axis=1)
    columns = jnp.concatenate(columns, axis=1)
    for a in range(2):
        rows = xy[a, :, :32].reshape(512, 128)
        cores = dot(rows, columns, TN)[64:]
        low = lower_half((64, 128))
        cores = [jnp.where(low, swap(core), core) for core in (cores[:, :128], cores[:, 128:])]
        cores = jnp.concatenate([jnp.concatenate(cores, axis=1), jnp.zeros((64, 256), F32)], axis=0)
        left = dot(rows, cores)
        high = left.astype(BF16)
        rest = (left - high.astype(F32)).astype(BF16)
        for b in range(2):
            lefts[a, b, :, :128] = high[:, 128 * b : 128 * b + 128]
            lefts[a, b, :, 128:] = rest[:, 128 * b : 128 * b + 128]
    for a in range(2):
        for part in range(4):
            for b in range(2):
                change = lax.dot_general(
                    lefts[a, b, 128 * part : 128 * part + 128], rights[b], NT, preferred_element_type=F32
                )
                for j in range(4):
                    lines = pl.ds(4096 * a + 1024 * part + 4 * b + j, 128, stride=8)
                    trail[lines, :] = trail[lines, :] - change[:, 128 * j : 128 * j + 128]

    for d in steps:
        at = (z + d) % 8
        copy(c_recv.at[at], c_recv.at[at], c_ss.at[0], c_rs.at[at], r, 2 * at + k).wait_recv()
    permuted = select_dot(unfold(c_recv), chosen[...], NN)
    coeffs[k] = pair_apply(permuted) * (512.0**-0.5)
    to_peer(4, coeffs.at[k], coeffs.at[k])

    from_peer(2, ranges.at[1 - k])
    from_peer(3, inverses.at[1 - k])
    from_peer(4, coeffs.at[1 - k])
    for one in sends:
        one.wait_send()


def finish_kernel(trail, ranges, coeffs, inverses, trail_out, basis_out, coeff_out, basis, coeff, sems):
    copies = [pltpu.make_async_copy(trail.at[pl.ds(2048 * i, 2048)], trail_out.at[pl.ds(2048 * i, 2048)], sems.at[i]) for i in range(4)]
    for one in copies:
        one.start()
    for a in range(2):
        inverse = inverses[a][:, :64]
        basis[a] = dot(inverse, ranges[a])
        coeff[a] = dot(inverse, coeffs[a])
    copies += [pltpu.make_async_copy(basis, basis_out, sems.at[4]), pltpu.make_async_copy(coeff, coeff_out, sems.at[5])]
    for one in copies[4:]:
        one.start()
    for one in copies:
        one.wait()


def body(n_row, trail, panel, row_basis, row_coeff, col_basis, col_scaled, pivot_basis, pivot_scaled, sketch, perm, pair_kind, pivot_values):
    turn = lambda x: jnp.swapaxes(x[:, 0], 1, 2)
    dma = pltpu.SemaphoreType.DMA
    inputs = (
        turn(panel),
        turn(row_basis),
        turn(row_coeff),
        pivot_basis.T,
        turn(col_basis),
        turn(col_scaled),
        sketch,
        perm.reshape(1, 512),
        pair_kind.reshape(1, 256),
        pivot_values,
        pivot_scaled,
    )
    small = jax.ShapeDtypeStruct((2, 64, 512), F32)
    results = pl.pallas_call(
        functools.partial(panel_kernel, n_row),
        out_shape=(
            jax.ShapeDtypeStruct((8192, 128), F32),
            small,
            small,
            jax.ShapeDtypeStruct((2, 64, 128), F32),
        ),
        in_specs=[HBM] * 12,
        out_specs=(VMEM,) * 4,
        scratch_shapes=[
            pltpu.VMEM((2, 16, 40, 128), F32),
            pltpu.VMEM((n_row, 2, 32, 128), F32),
            [pltpu.VMEM(x.shape, x.dtype) for x in inputs],
            pltpu.VMEM((2, 8, 16, 128), F32),
            pltpu.VMEM((16, 16, 128), F32),
            pltpu.VMEM((2, 32, 512), F32),
            pltpu.VMEM((512, 128), F32),
            pltpu.VMEM((2, 40, 128), F32),
            pltpu.VMEM((2, 32, 128), F32),
            pltpu.VMEM((32, 128), F32),
            pltpu.VMEM((8, 32, 128), F32),
            pltpu.VMEM((32, 128), F32),
            pltpu.VMEM((8, 32, 128), F32),
            pltpu.VMEM((512, 128), F32),
            pltpu.VMEM((512, 512), BF16),
            pltpu.VMEM((128, 512), F32),
            dma((16,)),
            dma((16,)),
            dma((16,)),
            dma((16,)),
            dma((n_row,)),
            dma((n_row,)),
            dma((8,)),
            dma((8,)),
            dma((8,)),
            dma((8,)),
            dma((5,)),
            dma((5,)),
            dma((11,)),
            dma(()),
            pltpu.VMEM((2, 2, 512, 256), BF16),
            pltpu.VMEM((2, 512, 256), BF16),
        ],
        compiler_params=pltpu.CompilerParams(
            collective_id=0, has_side_effects=True, vmem_limit_bytes=40 * 1024 * 1024
        ),
        name="panel",
    )(*[pltpu.with_memory_space_constraint(x, pltpu.HBM) for x in (trail.reshape(8192, 128), *inputs)])
    trail_out, basis_out, coeff_out = pl.pallas_call(
        finish_kernel,
        out_shape=(jax.ShapeDtypeStruct((8192, 128), F32), small, small),
        in_specs=[VMEM] * 4,
        out_specs=(HBM,) * 3,
        scratch_shapes=[pltpu.VMEM((2, 64, 512), F32), pltpu.VMEM((2, 64, 512), F32), dma((6,))],
        compiler_params=pltpu.CompilerParams(vmem_limit_bytes=40 * 1024 * 1024),
        name="finish",
    )(*results)
    return (trail_out.reshape(trail.shape), basis_out[:, None], coeff_out[:, None])


def solution(mesh):
    n_row = mesh.shape["row"]
    return jax.shard_map(
        functools.partial(body, n_row),
        mesh=mesh,
        in_specs=(
            P(None, "row", None, None, "col", None),
            P(None, "row", None, "col"),
            P(None, "row", None, "col"),
            P(None, "row", None, "col"),
            P(None, "col", None, "row"),
            P(None, "col", None, "row"),
            P(None, "col"),
            P(),
            P(),
            P(),
            P(),
            P(),
        ),
        out_specs=(
            P(None, "row", None, None, "col", None),
            P(None, "row", None, None),
            P(None, "row", None, None),
        ),
        check_vma=False,
    )
```

```python
import functools

import jax
import jax.numpy as jnp
from jax import lax
from jax.experimental import pallas as pl
from jax.experimental.pallas import tpu as pltpu
from jax.sharding import PartitionSpec as P

MESH = pl.DeviceIdType.MESH
F32 = jnp.float32
BF16 = jnp.bfloat16
HIGHEST = lax.Precision.HIGHEST
NN = (((1,), (0,)), ((), ()))
NT = (((1,), (1,)), ((), ()))
TN = (((0,), (0,)), ((), ()))
VMEM = pl.BlockSpec(memory_space=pltpu.VMEM)
HBM = pl.BlockSpec(memory_space=pltpu.HBM)


def dot(a, b, dims=NN):
    return lax.dot_general(a, b, dims, precision=HIGHEST, preferred_element_type=F32)


def split3(x):
    high = x.astype(BF16)
    rest = x - high.astype(F32)
    mid = rest.astype(BF16)
    low = (rest - mid.astype(F32)).astype(BF16)
    return jnp.concatenate([high, mid, low], axis=0)


def split2(x):
    high = x.astype(BF16)
    return high, (x - high.astype(F32)).astype(BF16)


def bdot(a, b, dims=NN):
    return lax.dot_general(a, b, dims, preferred_element_type=F32)


def select_dot(x, chosen, dims):
    n = x.shape[0]
    out = lax.dot_general(split3(x), chosen, dims, preferred_element_type=F32)
    return (out[2 * n :] + out[n : 2 * n]) + out[:n]


def lower_half(shape):
    return lax.broadcasted_iota(jnp.int32, shape, 1) % 128 < 64


def swap(x):
    return pltpu.roll(x, 64, 1)


def fold(x):
    return jnp.where(lower_half((32, 128)), x[:32], swap(x[32:]))


def unfold(ref):
    low = lower_half((32, 128))
    tops, bottoms = [], []
    for j in range(4):
        even, odd = ref[2 * j], ref[2 * j + 1]
        tops.append(jnp.where(low, even, swap(odd)))
        bottoms.append(jnp.where(low, swap(even), odd))
    return jnp.concatenate([jnp.concatenate(tops, axis=1), jnp.concatenate(bottoms, axis=1)], axis=0)


def inverse_factor(gram):
    rows = lax.broadcasted_iota(jnp.int32, (64, 64), 0)
    eye = (rows == lax.broadcasted_iota(jnp.int32, (64, 64), 1)).astype(F32)
    both = jnp.concatenate([gram, eye], axis=1)
    work = [both[8 * g : 8 * g + 8] for g in range(8)]
    sub = lax.broadcasted_iota(jnp.int32, (8, 128), 0)
    for k in range(8):
        columns = {
            (g, j): jnp.broadcast_to(work[g][:, 8 * k + j : 8 * k + j + 1], (8, 128))
            for g in range(k, 8)
            for j in range(8)
        }
        pivots = jnp.ones((8, 128), F32)
        for j in range(8):
            pivot = jnp.broadcast_to(columns[k, j][j : j + 1], (8, 128))
            pivots = jnp.where(sub == j, pivot, pivots)
            inverse = 1.0 / pivot
            scaled = jnp.broadcast_to(work[k][j : j + 1], (8, 128)) * inverse
            heads = {
                later: jnp.broadcast_to(columns[k, later][j : j + 1], (8, 128)) * inverse
                for later in range(j + 1, 8)
            }
            for g in range(k, 8):
                factor = columns[g, j]
                if g == k:
                    if j == 7:
                        continue
                    factor = jnp.where(sub > j, factor, 0.0)
                work[g] = work[g] - factor * scaled
                for later in range(j + 1, 8):
                    columns[g, later] = columns[g, later] - factor * heads[later]
        work[k] = work[k] * lax.rsqrt(pivots)
    return jnp.concatenate(work, axis=0)


def panel_kernel(
    n_row,
    trail_hbm,
    *refs,
):
    inputs, refs = refs[:11], refs[11:]
    run_panel(n_row, trail_hbm, inputs, *refs)


def run_panel(
    n_row,
    trail_hbm,
    inputs,
    trail,
    ranges,
    coeffs,
    inverses,
    xy,
    pb,
    zg,
    staged,
    pan_send,
    pan_recv,
    pan_chip,
    pan_full,
    xy_send,
    pb_send,
    zg_send,
    rng_send,
    rng_recv,
    c_send,
    c_recv,
    basis_full,
    chosen,
    updated,
    pan_ss,
    pan_rs,
    xy_ss,
    xy_rs,
    pb_ss,
    pb_rs,
    zx_ss,
    zx_rs,
    zy_ss,
    zy_rs,
    rng_ss,
    rng_rs,
    c_ss,
    c_rs,
    peer_ss,
    peer_rs,
    in_sem,
    trail_sem,
    lefts,
    rights,
):
    r = lax.axis_index("row")
    c = lax.axis_index("col")
    z = c // 2
    k = c % 2
    peer = 2 * z + 1 - k

    y, x = r // 4, r % 4
    order = [8, 9, 7, 10, 6, 11, 5, 12, 4, 13, 3, 14, 2, 15, 1]

    barrier = pltpu.get_barrier_semaphore()
    for d in order:
        pl.semaphore_signal(barrier, inc=1, device_id=(r, (c + d) % 16), device_id_type=MESH)
    for d in (2, 1, 3):
        pl.semaphore_signal(barrier, inc=1, device_id=(4 * y + (x + d) % 4, c), device_id_type=MESH)
        pl.semaphore_signal(barrier, inc=1, device_id=(4 * ((y + d) % 4) + x, c), device_id_type=MESH)
    loads = [pltpu.make_async_copy(src, dst, in_sem.at[i]) for i, (src, dst) in enumerate(zip(inputs, staged))]
    for one in loads:
        one.start()
    trail_load = pltpu.make_async_copy(trail_hbm, trail, trail_sem)
    panel, row_basis, row_coeff, pivot_basis, col_basis, col_scaled, sketch, perm, pair_kind, pivot_values, pivot_scaled = staged

    for one in loads:
        one.wait()
    low16 = lower_half((16, 128))
    for a in range(2):
        for j in range(4):
            tile = panel[a, :, 128 * j : 128 * j + 128]
            top, bottom = tile[:16], tile[16:]
            pan_send[a, 2 * j] = jnp.where(low16, top, swap(bottom))
            pan_send[a, 2 * j + 1] = jnp.where(low16, swap(top), bottom)
        xy_send[a, :, :64] = row_basis[a]
        xy_send[a, :, 64:] = row_coeff[a]
        pb_send[a, :, :64] = pivot_basis[16 * a : 16 * a + 8]
        pb_send[a, :, 64:] = pivot_basis[16 * a + 8 : 16 * a + 16]
        zg_send[a, :, :64] = col_basis[a]
        zg_send[a, :, 64:] = col_scaled[a]
    pan_recv[c] = pan_send[k, z]
    xy[k, c] = xy_send[k]
    pb[k, c] = pb_send[k]
    zg[r] = zg_send[...]
    pan_chip[k] = panel[k]

    pl.semaphore_wait(barrier, 21)

    def copy(src, dst, send_sem, recv_sem, row, col):
        return pltpu.make_async_remote_copy(
            src_ref=src,
            dst_ref=dst,
            send_sem=send_sem,
            recv_sem=recv_sem,
            device_id=(row, col),
            device_id_type=MESH,
        )

    sends = []

    def send(*args):
        one = copy(*args)
        one.start()
        sends.append(one)

    def to_peer(i, src, dst):
        send(src, dst, peer_ss.at[i], peer_rs.at[i], r, peer)

    def from_peer(i, ref):
        copy(ref, ref, peer_ss.at[i], peer_rs.at[i], r, peer).wait_recv()

    for d in order:
        to = (c + d) % 16
        send(pan_send.at[to % 2, to // 2], pan_recv.at[c], pan_ss.at[d], pan_rs.at[c], r, to)
    for d in (2, 1, 3):
        send(zg_send, zg.at[r], zx_ss.at[d], zx_rs.at[x], 4 * y + (x + d) % 4, c)
    for d in order:
        to = (c + d) % 16
        send(pb_send.at[to % 2], pb.at[to % 2, c], pb_ss.at[d], pb_rs.at[c], r, to)
    to_peer(0, panel.at[1 - k], pan_chip.at[k])
    for d in order:
        to = (c + d) % 16
        send(xy_send.at[to % 2], xy.at[to % 2, c], xy_ss.at[d], xy_rs.at[c], r, to)

    trail_load.start()
    q_ids = lax.broadcasted_iota(jnp.int32, (512, 512), 0)
    chosen[...] = (q_ids == perm[...]).astype(F32).astype(BF16)
    t_ids = lax.broadcasted_iota(jnp.int32, (256, 512), 1)
    spread = (t_ids // 2 == lax.broadcasted_iota(jnp.int32, (256, 512), 0)).astype(F32).astype(BF16)
    values = jnp.concatenate([pivot_values[...], pair_kind[...].astype(F32), jnp.zeros((4, 256), F32)], axis=0)
    values = select_dot(values, spread, NN)
    first, second, offdiag, twin = values[0:1], values[1:2], values[2:3], values[3:4] > 0.5
    odd = lax.broadcasted_iota(jnp.int32, (1, 512), 1) % 2 == 1
    own = jnp.where(odd, second, first)
    other = jnp.where(odd, first, second)
    determinant = first * second - offdiag * offdiag
    alpha = jnp.where(twin, other / determinant, 1.0 / own)
    beta = jnp.where(twin, -offdiag / determinant, 0.0)

    def pair_apply(x):
        partner = jnp.where(odd, pltpu.roll(x, 1, 1), pltpu.roll(x, 511, 1))
        return x * alpha + partner * beta

    scaled = select_dot(pair_apply(sketch[...]), chosen[...], NT)

    mine = pl.ds(pl.multiple_of(4 * y, 4), 4)
    for d in range(1, 4):
        at = (x + d) % 4
        copy(zg.at[4 * y + at], zg.at[4 * y + at], zx_ss.at[0], zx_rs.at[at], 4 * y + at, c).wait_recv()
    for d in (2, 1, 3):
        send(zg.at[mine], zg.at[mine], zy_ss.at[d], zy_rs.at[y], 4 * ((y + d) % 4) + x, c)
    for d in order:
        at = (c + d) % 16
        copy(pan_recv.at[at], pan_recv.at[at], pan_ss.at[0], pan_rs.at[at], r, at).wait_recv()
    for i in range(16):
        block = pan_recv[i]
        pan_full[32 * i : 32 * i + 16] = block
        pan_full[32 * i + 16 : 32 * i + 32] = swap(block)
    folded = fold(dot(scaled, pan_full[...]))
    rng_send[...] = folded
    rng_recv[z] = folded
    steps = [4, 5, 3, 6, 2, 7, 1]
    for d in steps:
        to = 2 * ((z + d) % 8) + k
        send(rng_send, rng_recv.at[z], rng_ss.at[d], rng_rs.at[z], r, to)

    for d in order:
        at = (c + d) % 16
        copy(pb.at[k, at], pb.at[k, at], pb_ss.at[0], pb_rs.at[at], r, at).wait_recv()
    to_peer(5, pb.at[k], pb.at[k])
    from_peer(0, pan_chip.at[1 - k])
    from_peer(5, pb.at[1 - k])
    for i in range(16):
        for half in range(2):
            block = pb[half, i]
            at = 32 * i + 16 * half
            basis_full[at : at + 8] = block
            basis_full[at + 8 : at + 16] = swap(block)
    weights = dot(scaled, basis_full[...])[:, :64]
    mine = basis_full[pl.ds(pl.multiple_of(64 * z, 64), 64), :][:, :64]
    mixer = dot(jnp.concatenate([weights, mine], axis=0), pivot_scaled[...])
    for d in order:
        at = (c + d) % 16
        copy(xy.at[k, at], xy.at[k, at], xy_ss.at[0], xy_rs.at[at], r, at).wait_recv()
    to_peer(1, xy.at[k], xy.at[k])
    left = xy[k].reshape(512, 128)
    mixed = dot(mixer, left)
    mixed = jnp.where(lower_half((128, 128)), swap(mixed), 0.0)
    fixes = dot(mixed, left, NT)
    updated[64:] = pan_chip[...].reshape(64, 512) - fixes[64:]

    for d in steps:
        at = (z + d) % 8
        copy(rng_recv.at[at], rng_recv.at[at], rng_ss.at[0], rng_rs.at[at], r, 2 * at + k).wait_recv()
    total = unfold(rng_recv) - fixes[:64]
    updated[:64] = total
    ranges[k] = total
    products = dot(total, updated[...], NT)
    folded = fold(swap(products))
    c_send[...] = folded
    c_recv[z] = folded
    for d in steps:
        to = 2 * ((z + d) % 8) + k
        send(c_send, c_recv.at[z], c_ss.at[d], c_rs.at[z], r, to)
    to_peer(2, ranges.at[k], ranges.at[k])

    inverses[k] = swap(inverse_factor(products[:, :64] * (1.0 / 512.0)))
    to_peer(3, inverses.at[k], inverses.at[k])
    from_peer(1, xy.at[1 - k])
    for d in range(1, 4):
        at = (y + d) % 4
        part = pl.ds(pl.multiple_of(4 * at, 4), 4)
        copy(zg.at[part], zg.at[part], zy_ss.at[0], zy_rs.at[at], 4 * at + x, c).wait_recv()
    trail_load.wait()
    low = lower_half((512, 128))
    columns = []
    for b in range(2):
        both = zg[:, b].reshape(512, 128)
        columns.append(both)
        twice = jnp.where(low, both, swap(both))
        high = twice.astype(BF16).astype(F32)
        pair = jnp.where(low, high, twice - high).astype(BF16)
        rights[b] = jnp.concatenate([pair, pair], axis=1)
    columns_high, columns_low = split2(jnp.concatenate(columns, axis=1))
    rows_high, rows_low = split2(jnp.concatenate([xy[0].reshape(512, 128), xy[1].reshape(512, 128)], axis=1))
    cores = bdot(rows_high, columns_low, TN) + bdot(rows_low, columns_high, TN) + bdot(rows_high, columns_high, TN)
    low = lower_half((64, 128))
    for a in range(2):
        core = cores[128 * a + 64 : 128 * a + 128]
        core = [jnp.where(low, swap(half), half) for half in (core[:, :128], core[:, 128:])]
        core = jnp.concatenate([jnp.concatenate(core, axis=1), jnp.zeros((64, 256), F32)], axis=0)
        core_high, core_low = split2(core)
        high, rest = rows_high[:, 128 * a : 128 * a + 128], rows_low[:, 128 * a : 128 * a + 128]
        left = bdot(high, core_low) + bdot(
            jnp.concatenate([high, rest], axis=1), jnp.concatenate([core_high, core_high], axis=0)
        )
        high, rest = split2(left)
        for b in range(2):
            lefts[a, b, :, :128] = high[:, 128 * b : 128 * b + 128]
            lefts[a, b, :, 128:] = rest[:, 128 * b : 128 * b + 128]

    def change(a, part):
        for b in range(2):
            delta = bdot(lefts[a, b, 128 * part : 128 * part + 128], rights[b], NT)
            for j in range(4):
                lines = pl.ds(4096 * a + 1024 * part + 4 * b + j, 128, stride=8)
                trail[lines, :] = trail[lines, :] - delta[:, 128 * j : 128 * j + 128]

    for part in range(4):
        change(0, part)

    for d in steps:
        at = (z + d) % 8
        copy(c_recv.at[at], c_recv.at[at], c_ss.at[0], c_rs.at[at], r, 2 * at + k).wait_recv()
    permuted = select_dot(unfold(c_recv), chosen[...], NN)
    coeffs[k] = pair_apply(permuted) * (512.0**-0.5)
    to_peer(4, coeffs.at[k], coeffs.at[k])
    for part in range(4):
        change(1, part)

    from_peer(2, ranges.at[1 - k])
    from_peer(3, inverses.at[1 - k])
    from_peer(4, coeffs.at[1 - k])
    for one in sends:
        one.wait_send()


def finish_kernel(trail, ranges, coeffs, inverses, trail_out, basis_out, coeff_out, basis, coeff, sems):
    copies = [pltpu.make_async_copy(trail.at[pl.ds(2048 * i, 2048)], trail_out.at[pl.ds(2048 * i, 2048)], sems.at[i]) for i in range(4)]
    for one in copies:
        one.start()
    for a in range(2):
        inverse = inverses[a][:, :64]
        basis[a] = dot(inverse, ranges[a])
        coeff[a] = dot(inverse, coeffs[a])
    copies += [pltpu.make_async_copy(basis, basis_out, sems.at[4]), pltpu.make_async_copy(coeff, coeff_out, sems.at[5])]
    for one in copies[4:]:
        one.start()
    for one in copies:
        one.wait()


def body(n_row, trail, panel, row_basis, row_coeff, col_basis, col_scaled, pivot_basis, pivot_scaled, sketch, perm, pair_kind, pivot_values):
    turn = lambda x: jnp.swapaxes(x[:, 0], 1, 2)
    dma = pltpu.SemaphoreType.DMA
    inputs = (
        turn(panel),
        turn(row_basis),
        turn(row_coeff),
        pivot_basis.T,
        turn(col_basis),
        turn(col_scaled),
        sketch,
        perm.reshape(1, 512),
        pair_kind.reshape(1, 256),
        pivot_values,
        pivot_scaled,
    )
    small = jax.ShapeDtypeStruct((2, 64, 512), F32)
    results = pl.pallas_call(
        functools.partial(panel_kernel, n_row),
        out_shape=(
            jax.ShapeDtypeStruct((8192, 128), F32),
            small,
            small,
            jax.ShapeDtypeStruct((2, 64, 128), F32),
        ),
        in_specs=[HBM] * 12,
        out_specs=(VMEM,) * 4,
        scratch_shapes=[
            pltpu.VMEM((2, 16, 32, 128), F32),
            pltpu.VMEM((2, 16, 8, 128), F32),
            pltpu.VMEM((n_row, 2, 32, 128), F32),
            [pltpu.VMEM(x.shape, x.dtype) for x in inputs],
            pltpu.VMEM((2, 8, 16, 128), F32),
            pltpu.VMEM((16, 16, 128), F32),
            pltpu.VMEM((2, 32, 512), F32),
            pltpu.VMEM((512, 128), F32),
            pltpu.VMEM((2, 32, 128), F32),
            pltpu.VMEM((2, 8, 128), F32),
            pltpu.VMEM((2, 32, 128), F32),
            pltpu.VMEM((32, 128), F32),
            pltpu.VMEM((8, 32, 128), F32),
            pltpu.VMEM((32, 128), F32),
            pltpu.VMEM((8, 32, 128), F32),
            pltpu.VMEM((512, 128), F32),
            pltpu.VMEM((512, 512), BF16),
            pltpu.VMEM((128, 512), F32),
            dma((16,)),
            dma((16,)),
            dma((16,)),
            dma((16,)),
            dma((16,)),
            dma((16,)),
            dma((4,)),
            dma((4,)),
            dma((4,)),
            dma((4,)),
            dma((8,)),
            dma((8,)),
            dma((8,)),
            dma((8,)),
            dma((6,)),
            dma((6,)),
            dma((11,)),
            dma(()),
            pltpu.VMEM((2, 2, 512, 256), BF16),
            pltpu.VMEM((2, 512, 256), BF16),
        ],
        compiler_params=pltpu.CompilerParams(
            collective_id=0, has_side_effects=True, vmem_limit_bytes=40 * 1024 * 1024
        ),
        name="panel",
    )(*[pltpu.with_memory_space_constraint(x, pltpu.HBM) for x in (trail.reshape(8192, 128), *inputs)])
    trail_out, basis_out, coeff_out = pl.pallas_call(
        finish_kernel,
        out_shape=(jax.ShapeDtypeStruct((8192, 128), F32), small, small),
        in_specs=[VMEM] * 4,
        out_specs=(HBM,) * 3,
        scratch_shapes=[pltpu.VMEM((2, 64, 512), F32), pltpu.VMEM((2, 64, 512), F32), dma((6,))],
        compiler_params=pltpu.CompilerParams(vmem_limit_bytes=40 * 1024 * 1024),
        name="finish",
    )(*results)
    return (trail_out.reshape(trail.shape), basis_out[:, None], coeff_out[:, None])


def solution(mesh):
    n_row = mesh.shape["row"]
    return jax.shard_map(
        functools.partial(body, n_row),
        mesh=mesh,
        in_specs=(
            P(None, "row", None, None, "col", None),
            P(None, "row", None, "col"),
            P(None, "row", None, "col"),
            P(None, "row", None, "col"),
            P(None, "col", None, "row"),
            P(None, "col", None, "row"),
            P(None, "col"),
            P(),
            P(),
            P(),
            P(),
            P(),
        ),
        out_specs=(
            P(None, "row", None, None, "col", None),
            P(None, "row", None, None),
            P(None, "row", None, None),
        ),
        check_vma=False,
    )
```

```python
import functools

import jax
import jax.numpy as jnp
from jax import lax
from jax.experimental import pallas as pl
from jax.experimental.pallas import tpu as pltpu
from jax.sharding import PartitionSpec as P

MESH = pl.DeviceIdType.MESH
F32 = jnp.float32
BF16 = jnp.bfloat16
HIGHEST = lax.Precision.HIGHEST
NN = (((1,), (0,)), ((), ()))
NT = (((1,), (1,)), ((), ()))
TN = (((0,), (0,)), ((), ()))
VMEM = pl.BlockSpec(memory_space=pltpu.VMEM)
HBM = pl.BlockSpec(memory_space=pltpu.HBM)


def dot(a, b, dims=NN):
    return lax.dot_general(a, b, dims, precision=HIGHEST, preferred_element_type=F32)


def split3(x):
    high = x.astype(BF16)
    rest = x - high.astype(F32)
    mid = rest.astype(BF16)
    low = (rest - mid.astype(F32)).astype(BF16)
    return jnp.concatenate([high, mid, low], axis=0)


def split2(x):
    high = x.astype(BF16)
    return high, (x - high.astype(F32)).astype(BF16)


def bdot(a, b, dims=NN):
    return lax.dot_general(a, b, dims, preferred_element_type=F32)


def select_dot(x, chosen, dims):
    n = x.shape[0]
    out = lax.dot_general(split3(x), chosen, dims, preferred_element_type=F32)
    return (out[2 * n :] + out[n : 2 * n]) + out[:n]


def lower_half(shape):
    return lax.broadcasted_iota(jnp.int32, shape, 1) % 128 < 64


def swap(x):
    return pltpu.roll(x, 64, 1)


def fold(x):
    return jnp.where(lower_half((32, 128)), x[:32], swap(x[32:]))


def unfold(ref):
    low = lower_half((32, 128))
    tops, bottoms = [], []
    for j in range(4):
        even, odd = ref[2 * j], ref[2 * j + 1]
        tops.append(jnp.where(low, even, swap(odd)))
        bottoms.append(jnp.where(low, swap(even), odd))
    return jnp.concatenate([jnp.concatenate(tops, axis=1), jnp.concatenate(bottoms, axis=1)], axis=0)


def inverse_factor(gram):
    rows = lax.broadcasted_iota(jnp.int32, (64, 64), 0)
    eye = (rows == lax.broadcasted_iota(jnp.int32, (64, 64), 1)).astype(F32)
    both = jnp.concatenate([gram, eye], axis=1)
    work = [both[8 * g : 8 * g + 8] for g in range(8)]
    sub = lax.broadcasted_iota(jnp.int32, (8, 128), 0)
    for k in range(8):
        columns = {
            (g, j): jnp.broadcast_to(work[g][:, 8 * k + j : 8 * k + j + 1], (8, 128))
            for g in range(k, 8)
            for j in range(8)
        }
        pivots = jnp.ones((8, 128), F32)
        for j in range(8):
            pivot = jnp.broadcast_to(columns[k, j][j : j + 1], (8, 128))
            pivots = jnp.where(sub == j, pivot, pivots)
            inverse = 1.0 / pivot
            scaled = jnp.broadcast_to(work[k][j : j + 1], (8, 128)) * inverse
            heads = {
                later: jnp.broadcast_to(columns[k, later][j : j + 1], (8, 128)) * inverse
                for later in range(j + 1, 8)
            }
            for g in range(k, 8):
                factor = columns[g, j]
                if g == k:
                    if j == 7:
                        continue
                    factor = jnp.where(sub > j, factor, 0.0)
                work[g] = work[g] - factor * scaled
                for later in range(j + 1, 8):
                    columns[g, later] = columns[g, later] - factor * heads[later]
        work[k] = work[k] * lax.rsqrt(pivots)
    return jnp.concatenate(work, axis=0)


def panel_kernel(
    n_row,
    trail_hbm,
    *refs,
):
    inputs, refs = refs[:11], refs[11:]
    run_panel(n_row, trail_hbm, inputs, *refs)


def run_panel(
    n_row,
    trail_hbm,
    inputs,
    trail,
    ranges,
    coeffs,
    inverses,
    xy,
    pb,
    zg,
    staged,
    pan_send,
    pan_recv,
    pan_chip,
    pan_full,
    xy_send,
    pb_send,
    zg_send,
    rng_send,
    rng_recv,
    c_send,
    c_recv,
    basis_full,
    chosen,
    updated,
    pan_sems,
    pb_sems,
    xy_far,
    xy_near,
    xy_relay,
    zx_sems,
    zy_sems,
    rng_sems,
    c_sems,
    peer_ss,
    peer_rs,
    in_sem,
    trail_sem,
    lefts,
    rights,
):
    r = lax.axis_index("row")
    c = lax.axis_index("col")
    z = c // 2
    k = c % 2
    peer = 2 * z + 1 - k

    y, x = r // 4, r % 4
    order = [8, 9, 7, 10, 6, 11, 5, 12, 4, 13, 3, 14, 2, 15, 1]

    barrier = pltpu.get_barrier_semaphore()
    for d in order:
        pl.semaphore_signal(barrier, inc=1, device_id=(r, (c + d) % 16), device_id_type=MESH)
    for d in (2, 1, 3):
        pl.semaphore_signal(barrier, inc=1, device_id=(4 * y + (x + d) % 4, c), device_id_type=MESH)
        pl.semaphore_signal(barrier, inc=1, device_id=(4 * ((y + d) % 4) + x, c), device_id_type=MESH)
    loads = [pltpu.make_async_copy(src, dst, in_sem.at[i]) for i, (src, dst) in enumerate(zip(inputs, staged))]
    for one in loads:
        one.start()
    trail_load = pltpu.make_async_copy(trail_hbm, trail, trail_sem)
    panel, row_basis, row_coeff, pivot_basis, col_basis, col_scaled, sketch, perm, pair_kind, pivot_values, pivot_scaled = staged

    for one in loads:
        one.wait()
    low16 = lower_half((16, 128))
    for a in range(2):
        for j in range(4):
            tile = panel[a, :, 128 * j : 128 * j + 128]
            top, bottom = tile[:16], tile[16:]
            pan_send[a, 2 * j] = jnp.where(low16, top, swap(bottom))
            pan_send[a, 2 * j + 1] = jnp.where(low16, swap(top), bottom)
        xy_send[a, :, :64] = row_basis[a]
        xy_send[a, :, 64:] = row_coeff[a]
        pb_send[a, :, :64] = pivot_basis[16 * a : 16 * a + 8]
        pb_send[a, :, 64:] = pivot_basis[16 * a + 8 : 16 * a + 16]
        zg_send[a, :, :64] = col_basis[a]
        zg_send[a, :, 64:] = col_scaled[a]
    pan_recv[c] = pan_send[k, z]
    xy[k, c] = xy_send[k]
    pb[k, c] = pb_send[k]
    zg[r] = zg_send[...]
    pan_chip[k] = panel[k]

    pl.semaphore_wait(barrier, 21)

    def copy(src, dst, send_sem, recv_sem, row, col):
        return pltpu.make_async_remote_copy(
            src_ref=src,
            dst_ref=dst,
            send_sem=send_sem,
            recv_sem=recv_sem,
            device_id=(row, col),
            device_id_type=MESH,
        )

    def send(src, dst, sems, row, col):
        copy(src, dst, sems.at[0], sems.at[1], row, col).start()

    def landed(ref, sems):
        copy(ref, ref, sems.at[0], sems.at[1], r, peer).wait_recv()

    def sent(ref, sems):
        copy(ref, ref, sems.at[0], sems.at[1], r, peer).wait_send()

    peer_copies = []

    def to_peer(i, src, dst):
        one = copy(src, dst, peer_ss.at[i], peer_rs.at[i], r, peer)
        one.start()
        peer_copies.append(one)

    def from_peer(i, ref):
        copy(ref, ref, peer_ss.at[i], peer_rs.at[i], r, peer).wait_recv()

    for d in order:
        to = (c + d) % 16
        send(pan_send.at[to % 2, to // 2], pan_recv.at[c], pan_sems, r, to)
    for d in (2, 1, 3):
        send(zg_send, zg.at[r], zx_sems, 4 * y + (x + d) % 4, c)
    for d in order:
        to = (c + d) % 16
        send(pb_send.at[to % 2], pb.at[to % 2, c], pb_sems, r, to)
    to_peer(0, panel.at[1 - k], pan_chip.at[k])
    for d in (2, 6, 1, 7):
        for core in range(2):
            to = 2 * ((z + d) % 8) + core
            send(xy_send.at[core], xy.at[core, c], xy_far if d in (2, 6) else xy_near, r, to)
    send(xy_send.at[1 - k], xy.at[1 - k, c], xy_near, r, peer)

    trail_load.start()
    q_ids = lax.broadcasted_iota(jnp.int32, (512, 512), 0)
    chosen[...] = (q_ids == perm[...]).astype(F32).astype(BF16)
    t_ids = lax.broadcasted_iota(jnp.int32, (256, 512), 1)
    spread = (t_ids // 2 == lax.broadcasted_iota(jnp.int32, (256, 512), 0)).astype(F32).astype(BF16)
    values = jnp.concatenate([pivot_values[...], pair_kind[...].astype(F32), jnp.zeros((4, 256), F32)], axis=0)
    values = select_dot(values, spread, NN)
    first, second, offdiag, twin = values[0:1], values[1:2], values[2:3], values[3:4] > 0.5
    odd = lax.broadcasted_iota(jnp.int32, (1, 512), 1) % 2 == 1
    own = jnp.where(odd, second, first)
    other = jnp.where(odd, first, second)
    determinant = first * second - offdiag * offdiag
    alpha = jnp.where(twin, other / determinant, 1.0 / own)
    beta = jnp.where(twin, -offdiag / determinant, 0.0)

    def pair_apply(x):
        partner = jnp.where(odd, pltpu.roll(x, 1, 1), pltpu.roll(x, 511, 1))
        return x * alpha + partner * beta

    scaled = select_dot(pair_apply(sketch[...]), chosen[...], NT)

    mine = pl.ds(pl.multiple_of(4 * y, 4), 4)
    landed(zg.at[pl.ds(0, 3)], zx_sems)
    for d in (2, 1, 3):
        send(zg.at[mine], zg.at[mine], zy_sems, 4 * ((y + d) % 4) + x, c)
    landed(pan_recv.at[pl.ds(0, 15)], pan_sems)
    for i in range(16):
        block = pan_recv[i]
        pan_full[32 * i : 32 * i + 16] = block
        pan_full[32 * i + 16 : 32 * i + 32] = swap(block)
    folded = fold(dot(scaled, pan_full[...]))
    rng_send[...] = folded
    rng_recv[z] = folded
    steps = [4, 5, 3, 6, 2, 7, 1]
    for d in steps:
        to = 2 * ((z + d) % 8) + k
        send(rng_send, rng_recv.at[z], rng_sems, r, to)

    landed(xy.at[0, pl.ds(0, 4)], xy_far)
    for d, side in ((6, 1), (2, -1)):
        origin = 2 * ((z + d) % 8)
        both = xy.at[k, pl.ds(pl.multiple_of(origin, 2), 2)]
        send(both, both, xy_relay, r, 2 * ((z + side) % 8) + k)
        one = xy.at[k, origin + (d == 2)]
        send(one, one, xy_relay, r, 2 * ((z + 2 * side) % 8) + k)
    landed(pb.at[0, pl.ds(0, 15)], pb_sems)
    to_peer(5, pb.at[k], pb.at[k])
    from_peer(0, pan_chip.at[1 - k])
    from_peer(5, pb.at[1 - k])
    for i in range(16):
        for half in range(2):
            block = pb[half, i]
            at = 32 * i + 16 * half
            basis_full[at : at + 8] = block
            basis_full[at + 8 : at + 16] = swap(block)
    weights = dot(scaled, basis_full[...])[:, :64]
    mine = basis_full[pl.ds(pl.multiple_of(64 * z, 64), 64), :][:, :64]
    mixer = dot(jnp.concatenate([weights, mine], axis=0), pivot_scaled[...])
    landed(xy.at[0, pl.ds(0, 5)], xy_near)
    landed(xy.at[0, pl.ds(0, 6)], xy_relay)
    to_peer(1, xy.at[k], xy.at[k])
    left = xy[k].reshape(512, 128)
    mixed = dot(mixer, left)
    mixed = jnp.where(lower_half((128, 128)), swap(mixed), 0.0)
    fixes = dot(mixed, left, NT)
    updated[64:] = pan_chip[...].reshape(64, 512) - fixes[64:]

    landed(rng_recv.at[pl.ds(0, 7)], rng_sems)
    total = unfold(rng_recv) - fixes[:64]
    updated[:64] = total
    ranges[k] = total
    products = dot(total, updated[...], NT)
    folded = fold(swap(products))
    c_send[...] = folded
    c_recv[z] = folded
    for d in steps:
        to = 2 * ((z + d) % 8) + k
        send(c_send, c_recv.at[z], c_sems, r, to)
    to_peer(2, ranges.at[k], ranges.at[k])

    @pl.when(c < 16)
    def _():
        inverses[k] = swap(inverse_factor(products[:, :64] * (1.0 / 512.0)))

    to_peer(3, inverses.at[k], inverses.at[k])
    from_peer(1, xy.at[1 - k])
    landed(zg.at[pl.ds(0, 12)], zy_sems)
    trail_load.wait()
    low = lower_half((512, 128))
    columns = []
    for b in range(2):
        both = zg[:, b].reshape(512, 128)
        columns.append(both)
        twice = jnp.where(low, both, swap(both))
        high = twice.astype(BF16).astype(F32)
        pair = jnp.where(low, high, twice - high).astype(BF16)
        rights[b] = jnp.concatenate([pair, pair], axis=1)
    columns_high, columns_low = split2(jnp.concatenate(columns, axis=1))
    rows_high, rows_low = split2(jnp.concatenate([xy[0].reshape(512, 128), xy[1].reshape(512, 128)], axis=1))
    cores = bdot(rows_high, columns_low, TN) + bdot(rows_low, columns_high, TN) + bdot(rows_high, columns_high, TN)
    low = lower_half((64, 128))
    for a in range(2):
        core = cores[128 * a + 64 : 128 * a + 128]
        core = [jnp.where(low, swap(half), half) for half in (core[:, :128], core[:, 128:])]
        core = jnp.concatenate([jnp.concatenate(core, axis=1), jnp.zeros((64, 256), F32)], axis=0)
        core_high, core_low = split2(core)
        high, rest = rows_high[:, 128 * a : 128 * a + 128], rows_low[:, 128 * a : 128 * a + 128]
        left = bdot(high, core_low) + bdot(
            jnp.concatenate([high, rest], axis=1), jnp.concatenate([core_high, core_high], axis=0)
        )
        high, rest = split2(left)
        for b in range(2):
            lefts[a, b, :, :128] = high[:, 128 * b : 128 * b + 128]
            lefts[a, b, :, 128:] = rest[:, 128 * b : 128 * b + 128]

    def change(a):
        @pl.loop(0, 4)
        def _(part):
            for b in range(2):
                delta = bdot(lefts[a, b, pl.ds(pl.multiple_of(128 * part, 128), 128)], rights[b], NT)
                for j in range(4):
                    lines = pl.ds(pl.multiple_of(4096 * a + 1024 * part, 1024) + 4 * b + j, 128, stride=8)
                    trail[lines, :] = trail[lines, :] - delta[:, 128 * j : 128 * j + 128]

    change(0)

    landed(c_recv.at[pl.ds(0, 7)], c_sems)
    permuted = select_dot(unfold(c_recv), chosen[...], NN)
    coeffs[k] = pair_apply(permuted) * (512.0**-0.5)
    to_peer(4, coeffs.at[k], coeffs.at[k])
    change(1)

    from_peer(2, ranges.at[1 - k])
    from_peer(3, inverses.at[1 - k])
    from_peer(4, coeffs.at[1 - k])
    for one in peer_copies:
        one.wait_send()
    sent(pan_recv.at[pl.ds(0, 15)], pan_sems)
    sent(pb.at[0, pl.ds(0, 15)], pb_sems)
    sent(xy.at[0, pl.ds(0, 4)], xy_far)
    sent(xy.at[0, pl.ds(0, 5)], xy_near)
    sent(xy.at[0, pl.ds(0, 6)], xy_relay)
    sent(zg.at[pl.ds(0, 3)], zx_sems)
    sent(zg.at[pl.ds(0, 12)], zy_sems)
    sent(rng_recv.at[pl.ds(0, 7)], rng_sems)
    sent(c_recv.at[pl.ds(0, 7)], c_sems)


def finish_kernel(trail, ranges, coeffs, inverses, trail_out, basis_out, coeff_out, basis, coeff, sems):
    copies = [pltpu.make_async_copy(trail.at[pl.ds(2048 * i, 2048)], trail_out.at[pl.ds(2048 * i, 2048)], sems.at[i]) for i in range(4)]
    for one in copies:
        one.start()
    for a in range(2):
        inverse = inverses[a][:, :64]
        basis[a] = dot(inverse, ranges[a])
        coeff[a] = dot(inverse, coeffs[a])
    copies += [pltpu.make_async_copy(basis, basis_out, sems.at[4]), pltpu.make_async_copy(coeff, coeff_out, sems.at[5])]
    for one in copies[4:]:
        one.start()
    for one in copies:
        one.wait()


def body(n_row, trail, panel, row_basis, row_coeff, col_basis, col_scaled, pivot_basis, pivot_scaled, sketch, perm, pair_kind, pivot_values):
    turn = lambda x: jnp.swapaxes(x[:, 0], 1, 2)
    dma = pltpu.SemaphoreType.DMA
    inputs = (
        turn(panel),
        turn(row_basis),
        turn(row_coeff),
        pivot_basis.T,
        turn(col_basis),
        turn(col_scaled),
        sketch,
        perm.reshape(1, 512),
        pair_kind.reshape(1, 256),
        pivot_values,
        pivot_scaled,
    )
    small = jax.ShapeDtypeStruct((2, 64, 512), F32)
    results = pl.pallas_call(
        functools.partial(panel_kernel, n_row),
        out_shape=(
            jax.ShapeDtypeStruct((8192, 128), F32),
            small,
            small,
            jax.ShapeDtypeStruct((2, 64, 128), F32),
        ),
        in_specs=[HBM] * 12,
        out_specs=(VMEM,) * 4,
        scratch_shapes=[
            pltpu.VMEM((2, 16, 32, 128), F32),
            pltpu.VMEM((2, 16, 8, 128), F32),
            pltpu.VMEM((n_row, 2, 32, 128), F32),
            [pltpu.VMEM(x.shape, x.dtype) for x in inputs],
            pltpu.VMEM((2, 8, 16, 128), F32),
            pltpu.VMEM((16, 16, 128), F32),
            pltpu.VMEM((2, 32, 512), F32),
            pltpu.VMEM((512, 128), F32),
            pltpu.VMEM((2, 32, 128), F32),
            pltpu.VMEM((2, 8, 128), F32),
            pltpu.VMEM((2, 32, 128), F32),
            pltpu.VMEM((32, 128), F32),
            pltpu.VMEM((8, 32, 128), F32),
            pltpu.VMEM((32, 128), F32),
            pltpu.VMEM((8, 32, 128), F32),
            pltpu.VMEM((512, 128), F32),
            pltpu.VMEM((512, 512), BF16),
            pltpu.VMEM((128, 512), F32),
            *[dma((2,))] * 9,
            dma((6,)),
            dma((6,)),
            dma((11,)),
            dma(()),
            pltpu.VMEM((2, 2, 512, 256), BF16),
            pltpu.VMEM((2, 512, 256), BF16),
        ],
        compiler_params=pltpu.CompilerParams(
            collective_id=0, has_side_effects=True, vmem_limit_bytes=40 * 1024 * 1024
        ),
        name="panel",
    )(*[pltpu.with_memory_space_constraint(x, pltpu.HBM) for x in (trail.reshape(8192, 128), *inputs)])
    trail_out, basis_out, coeff_out = pl.pallas_call(
        finish_kernel,
        out_shape=(jax.ShapeDtypeStruct((8192, 128), F32), small, small),
        in_specs=[VMEM] * 4,
        out_specs=(HBM,) * 3,
        scratch_shapes=[pltpu.VMEM((2, 64, 512), F32), pltpu.VMEM((2, 64, 512), F32), dma((6,))],
        compiler_params=pltpu.CompilerParams(vmem_limit_bytes=40 * 1024 * 1024),
        name="finish",
    )(*results)
    return (trail_out.reshape(trail.shape), basis_out[:, None], coeff_out[:, None])


def solution(mesh):
    n_row = mesh.shape["row"]
    return jax.shard_map(
        functools.partial(body, n_row),
        mesh=mesh,
        in_specs=(
            P(None, "row", None, None, "col", None),
            P(None, "row", None, "col"),
            P(None, "row", None, "col"),
            P(None, "row", None, "col"),
            P(None, "col", None, "row"),
            P(None, "col", None, "row"),
            P(None, "col"),
            P(),
            P(),
            P(),
            P(),
            P(),
        ),
        out_specs=(
            P(None, "row", None, None, "col", None),
            P(None, "row", None, None),
            P(None, "row", None, None),
        ),
        check_vma=False,
    )
```

```python
import functools

import jax
import jax.numpy as jnp
from jax import lax
from jax.experimental import pallas as pl
from jax.experimental.pallas import tpu as pltpu
from jax.sharding import PartitionSpec as P

MESH = pl.DeviceIdType.MESH
F32 = jnp.float32
BF16 = jnp.bfloat16
HIGHEST = lax.Precision.HIGHEST
NN = (((1,), (0,)), ((), ()))
NT = (((1,), (1,)), ((), ()))
TN = (((0,), (0,)), ((), ()))
VMEM = pl.BlockSpec(memory_space=pltpu.VMEM)
HBM = pl.BlockSpec(memory_space=pltpu.HBM)


def dot(a, b, dims=NN):
    return lax.dot_general(a, b, dims, precision=HIGHEST, preferred_element_type=F32)


def split3(x):
    high = x.astype(BF16)
    rest = x - high.astype(F32)
    mid = rest.astype(BF16)
    low = (rest - mid.astype(F32)).astype(BF16)
    return jnp.concatenate([high, mid, low], axis=0)


def split2(x):
    high = x.astype(BF16)
    return high, (x - high.astype(F32)).astype(BF16)


def bdot(a, b, dims=NN):
    return lax.dot_general(a, b, dims, preferred_element_type=F32)


def select_dot(x, chosen, dims):
    n = x.shape[0]
    out = lax.dot_general(split3(x), chosen, dims, preferred_element_type=F32)
    return (out[2 * n :] + out[n : 2 * n]) + out[:n]


def lower_half(shape):
    return lax.broadcasted_iota(jnp.int32, shape, 1) % 128 < 64


def swap(x):
    return pltpu.roll(x, 64, 1)


def fold(x):
    return jnp.where(lower_half((32, 128)), x[:32], swap(x[32:]))


def unfold(ref):
    low = lower_half((32, 128))
    tops, bottoms = [], []
    for j in range(4):
        even, odd = ref[2 * j], ref[2 * j + 1]
        tops.append(jnp.where(low, even, swap(odd)))
        bottoms.append(jnp.where(low, swap(even), odd))
    return jnp.concatenate([jnp.concatenate(tops, axis=1), jnp.concatenate(bottoms, axis=1)], axis=0)


def pair_apply(x, factors):
    odd = lax.broadcasted_iota(jnp.int32, x.shape, 1) % 2 == 1
    partner = jnp.where(odd, pltpu.roll(x, 1, 1), pltpu.roll(x, 511, 1))
    return x * factors[0:1] + partner * factors[1:2]


def inverse_factor(gram):
    rows = lax.broadcasted_iota(jnp.int32, (64, 64), 0)
    eye = (rows == lax.broadcasted_iota(jnp.int32, (64, 64), 1)).astype(F32)
    both = jnp.concatenate([gram, eye], axis=1)
    work = [both[8 * g : 8 * g + 8] for g in range(8)]
    sub = lax.broadcasted_iota(jnp.int32, (8, 128), 0)
    for k in range(8):
        columns = {
            (g, j): jnp.broadcast_to(work[g][:, 8 * k + j : 8 * k + j + 1], (8, 128))
            for g in range(k, 8)
            for j in range(8)
        }
        pivots = jnp.ones((8, 128), F32)
        for j in range(8):
            pivot = jnp.broadcast_to(columns[k, j][j : j + 1], (8, 128))
            pivots = jnp.where(sub == j, pivot, pivots)
            inverse = 1.0 / pivot
            scaled = jnp.broadcast_to(work[k][j : j + 1], (8, 128)) * inverse
            heads = {
                later: jnp.broadcast_to(columns[k, later][j : j + 1], (8, 128)) * inverse
                for later in range(j + 1, 8)
            }
            for g in range(k, 8):
                factor = columns[g, j]
                if g == k:
                    if j == 7:
                        continue
                    factor = jnp.where(sub > j, factor, 0.0)
                work[g] = work[g] - factor * scaled
                for later in range(j + 1, 8):
                    columns[g, later] = columns[g, later] - factor * heads[later]
        work[k] = work[k] * lax.rsqrt(pivots)
    return jnp.concatenate(work, axis=0)


def panel_kernel(
    n_row,
    trail_hbm,
    *refs,
):
    inputs, refs = refs[:11], refs[11:]
    run_panel(n_row, trail_hbm, inputs, *refs)


def run_panel(
    n_row,
    trail_hbm,
    inputs,
    trail,
    bases,
    inverses,
    crosses,
    chosen,
    factors,
    xy,
    pb,
    zg,
    staged,
    pan_send,
    pan_recv,
    pan_chip,
    pan_full,
    xy_send,
    pb_send,
    zg_send,
    rng_send,
    rng_recv,
    c_send,
    basis_full,
    panel_high,
    panel_low,
    ranges,
    pan_sems,
    pb_sems,
    px_sems,
    xy_far,
    xy_near,
    xy_relay,
    zx_sems,
    zy_sems,
    rng_sems,
    c_sems,
    peer_ss,
    peer_rs,
    in_sem,
    trail_sem,
    lefts,
    rights,
):
    r = lax.axis_index("row")
    c = lax.axis_index("col")
    z = c // 2
    k = c % 2
    peer = 2 * z + 1 - k

    y, x = r // 4, r % 4
    order = [8, 9, 7, 10, 6, 11, 5, 12, 4, 13, 3, 14, 2, 15, 1]

    steps = [4, 5, 3, 6, 2, 7, 1]

    barrier = pltpu.get_barrier_semaphore()
    for d in order:
        pl.semaphore_signal(barrier, inc=1, device_id=(r, (c + d) % 16), device_id_type=MESH)
    for d in (2, 1, 3):
        pl.semaphore_signal(barrier, inc=1, device_id=(4 * y + (x + d) % 4, c), device_id_type=MESH)
        pl.semaphore_signal(barrier, inc=1, device_id=(4 * ((y + d) % 4) + x, c), device_id_type=MESH)
    loads = [pltpu.make_async_copy(src, dst, in_sem.at[i]) for i, (src, dst) in enumerate(zip(inputs, staged))]
    for one in loads:
        one.start()
    trail_load = pltpu.make_async_copy(trail_hbm, trail, trail_sem)
    panel, row_basis, row_coeff, pivot_basis, col_basis, col_scaled, sketch, perm, pair_kind, pivot_values, pivot_scaled = staged

    for one in loads:
        one.wait()
    low16 = lower_half((16, 128))
    for a in range(2):
        for j in range(4):
            tile = panel[a, :, 128 * j : 128 * j + 128]
            top, bottom = tile[:16], tile[16:]
            pan_send[a, 2 * j] = jnp.where(low16, top, swap(bottom))
            pan_send[a, 2 * j + 1] = jnp.where(low16, swap(top), bottom)
        xy_send[a, :, :64] = row_basis[a]
        xy_send[a, :, 64:] = row_coeff[a]
        pb_send[a, :, :64] = pivot_basis[16 * a : 16 * a + 8]
        pb_send[a, :, 64:] = pivot_basis[16 * a + 8 : 16 * a + 16]
        zg_send[a, :, :64] = col_basis[a]
        zg_send[a, :, 64:] = col_scaled[a]
    pan_recv[c] = pan_send[k, z]
    xy[k, c] = xy_send[k]
    pb[k, x % 2, z] = pb_send[x % 2]
    zg[r] = zg_send[...]
    pan_chip[k] = panel[k]

    pl.semaphore_wait(barrier, 21)

    def copy(src, dst, send_sem, recv_sem, row, col):
        return pltpu.make_async_remote_copy(
            src_ref=src,
            dst_ref=dst,
            send_sem=send_sem,
            recv_sem=recv_sem,
            device_id=(row, col),
            device_id_type=MESH,
        )

    def send(src, dst, sems, row, col):
        copy(src, dst, sems.at[0], sems.at[1], row, col).start()

    def landed(ref, sems):
        copy(ref, ref, sems.at[0], sems.at[1], r, peer).wait_recv()

    def sent(ref, sems):
        copy(ref, ref, sems.at[0], sems.at[1], r, peer).wait_send()

    peer_copies = []

    def to_peer(i, src, dst):
        one = copy(src, dst, peer_ss.at[i], peer_rs.at[i], r, peer)
        one.start()
        peer_copies.append(one)

    def from_peer(i, ref):
        copy(ref, ref, peer_ss.at[i], peer_rs.at[i], r, peer).wait_recv()

    for d in order:
        to = (c + d) % 16
        send(pan_send.at[to % 2, to // 2], pan_recv.at[c], pan_sems, r, to)
    for d in (2, 1, 3):
        send(zg_send, zg.at[r], zx_sems, 4 * y + (x + d) % 4, c)
    for d in steps:
        send(pb_send.at[x % 2], pb.at[k, x % 2, z], pb_sems, r, 2 * ((z + d) % 8) + k)
    to_peer(0, panel.at[1 - k], pan_chip.at[k])
    for d in (2, 6, 1, 7):
        for core in range(2):
            to = 2 * ((z + d) % 8) + core
            send(xy_send.at[core], xy.at[core, c], xy_far if d in (2, 6) else xy_near, r, to)
    send(xy_send.at[1 - k], xy.at[1 - k, c], xy_near, r, peer)

    trail_load.start()
    q_ids = lax.broadcasted_iota(jnp.int32, (512, 512), 0)
    chosen[...] = (q_ids == perm[...]).astype(F32).astype(BF16)
    t_ids = lax.broadcasted_iota(jnp.int32, (256, 512), 1)
    spread = (t_ids // 2 == lax.broadcasted_iota(jnp.int32, (256, 512), 0)).astype(F32).astype(BF16)
    values = jnp.concatenate([pivot_values[...], pair_kind[...].astype(F32), jnp.zeros((4, 256), F32)], axis=0)
    values = select_dot(values, spread, NN)
    first, second, offdiag, twin = values[0:1], values[1:2], values[2:3], values[3:4] > 0.5
    odd = lax.broadcasted_iota(jnp.int32, (1, 512), 1) % 2 == 1
    own = jnp.where(odd, second, first)
    other = jnp.where(odd, first, second)
    determinant = first * second - offdiag * offdiag
    alpha = jnp.where(twin, other / determinant, 1.0 / own)
    beta = jnp.where(twin, -offdiag / determinant, 0.0)

    factors[...] = jnp.concatenate([alpha, beta, jnp.zeros((6, 512), F32)], axis=0)
    scaled = select_dot(pair_apply(sketch[...], factors), chosen[...], NT)

    mine = pl.ds(pl.multiple_of(4 * y, 4), 4)
    landed(zg.at[pl.ds(0, 3)], zx_sems)
    for d in (2, 1, 3):
        send(zg.at[mine], zg.at[mine], zy_sems, 4 * ((y + d) % 4) + x, c)
    landed(pan_recv.at[pl.ds(0, 15)], pan_sems)
    for i in range(16):
        block = pan_recv[i]
        pan_full[32 * i : 32 * i + 16] = block
        pan_full[32 * i + 16 : 32 * i + 32] = swap(block)
    folded = fold(dot(scaled, pan_full[...]))
    rng_send[...] = folded
    rng_recv[z] = folded
    for d in steps:
        to = 2 * ((z + d) % 8) + k
        send(rng_send, rng_recv.at[z], rng_sems, r, to)

    landed(pb.at[0, 0, pl.ds(0, 7)], pb_sems)
    send(pb.at[k, x % 2], pb.at[k, x % 2], px_sems, 4 * y + x + 1 - 2 * (x % 2), c)
    landed(xy.at[0, pl.ds(0, 4)], xy_far)
    for d, side in ((6, 1), (2, -1)):
        origin = 2 * ((z + d) % 8)
        both = xy.at[k, pl.ds(pl.multiple_of(origin, 2), 2)]
        send(both, both, xy_relay, r, 2 * ((z + side) % 8) + k)
        one = xy.at[k, origin + (d == 2)]
        send(one, one, xy_relay, r, 2 * ((z + 2 * side) % 8) + k)
    landed(pb.at[0, 0], px_sems)
    to_peer(5, pb.at[k], pb.at[k])
    from_peer(0, pan_chip.at[1 - k])
    from_peer(5, pb.at[1 - k])
    for i in range(16):
        for half in range(2):
            block = pb[i % 2, half, i // 2]
            at = 32 * i + 16 * half
            basis_full[at : at + 8] = block
            basis_full[at + 8 : at + 16] = swap(block)
    weights = dot(scaled, basis_full[...])[:, :64]
    mine = basis_full[pl.ds(pl.multiple_of(64 * z, 64), 64), :][:, :64]
    mixer = dot(jnp.concatenate([weights, mine], axis=0), pivot_scaled[...])
    mixer_high, mixer_low = split2(mixer)
    mixer_both = jnp.concatenate([mixer_high, mixer_low], axis=0)
    landed(xy.at[0, pl.ds(0, 5)], xy_near)
    landed(xy.at[0, pl.ds(0, 6)], xy_relay)
    to_peer(1, xy.at[k], xy.at[k])
    left_high, left_low = split2(xy[k].reshape(512, 128))
    mixed = bdot(mixer_both, left_high)
    mixed = (bdot(mixer_high, left_low) + mixed[128:]) + mixed[:128]
    mixed = jnp.where(lower_half((128, 128)), swap(mixed), 0.0)
    mixed_high, mixed_low = split2(mixed)
    fixes = bdot(mixed_high, left_low, NT) + bdot(
        jnp.concatenate([mixed_high, mixed_low], axis=1), jnp.concatenate([left_high, left_high], axis=1), NT
    )
    panel_high[...], panel_low[...] = split2(pan_chip[...].reshape(64, 512) - fixes[64:])

    landed(rng_recv.at[pl.ds(0, 7)], rng_sems)
    total = unfold(rng_recv) - fixes[:64]
    ranges[...] = total
    total_high, total_low = split2(total)
    cross = bdot(jnp.concatenate([total_high, total_low], axis=0), panel_high[...], NT)
    cross = (bdot(total_high, panel_low[...], NT) + cross[64:]) + cross[:64]
    cross = jnp.concatenate([cross, cross], axis=1)
    folded = jnp.where(lower_half((32, 128)), cross[:32], cross[32:])
    c_send[...] = folded
    crosses[k, z] = folded
    for d in steps:
        to = 2 * ((z + d) % 8) + k
        send(c_send, crosses.at[k, z], c_sems, r, to)

    @pl.when(c < 16)
    def _():
        total = ranges[...]
        inverse = swap(inverse_factor(dot(total, total, NT) * (1.0 / 512.0)))
        inverses[k] = inverse
        bases[k] = dot(inverse[:, :64], total)

    to_peer(2, bases.at[k], bases.at[k])
    to_peer(3, inverses.at[k], inverses.at[k])
    from_peer(1, xy.at[1 - k])
    landed(zg.at[pl.ds(0, 12)], zy_sems)
    trail_load.wait()
    low = lower_half((512, 128))
    columns = []
    for b in range(2):
        both = zg[:, b].reshape(512, 128)
        columns.append(both)
        twice = jnp.where(low, both, swap(both))
        high = twice.astype(BF16).astype(F32)
        pair = jnp.where(low, high, twice - high).astype(BF16)
        rights[b] = jnp.concatenate([pair, pair], axis=1)
    columns_high, columns_low = split2(jnp.concatenate(columns, axis=1))
    rows_high, rows_low = split2(jnp.concatenate([xy[0].reshape(512, 128), xy[1].reshape(512, 128)], axis=1))
    cores = bdot(rows_high, columns_low, TN) + bdot(rows_low, columns_high, TN) + bdot(rows_high, columns_high, TN)
    low = lower_half((64, 128))
    for a in range(2):
        core = cores[128 * a + 64 : 128 * a + 128]
        core = [jnp.where(low, swap(half), half) for half in (core[:, :128], core[:, 128:])]
        core = jnp.concatenate([jnp.concatenate(core, axis=1), jnp.zeros((64, 256), F32)], axis=0)
        core_high, core_low = split2(core)
        high, rest = rows_high[:, 128 * a : 128 * a + 128], rows_low[:, 128 * a : 128 * a + 128]
        left = bdot(high, core_low) + bdot(
            jnp.concatenate([high, rest], axis=1), jnp.concatenate([core_high, core_high], axis=0)
        )
        high, rest = split2(left)
        for b in range(2):
            lefts[a, b, :, :128] = high[:, 128 * b : 128 * b + 128]
            lefts[a, b, :, 128:] = rest[:, 128 * b : 128 * b + 128]

    def change(a, parts):
        @pl.when(c < 16)
        def _():
            for part in parts:
                for b in range(2):
                    delta = bdot(lefts[a, b, 128 * part : 128 * part + 128], rights[b], NT)
                    for j in range(4):
                        lines = pl.ds(4096 * a + 1024 * part + 4 * b + j, 128, stride=8)
                        trail[lines, :] = trail[lines, :] - delta[:, 128 * j : 128 * j + 128]

    change(0, range(4))

    landed(crosses.at[0, pl.ds(0, 7)], c_sems)
    to_peer(4, crosses.at[k], crosses.at[k])
    change(1, range(4))
    from_peer(2, bases.at[1 - k])
    from_peer(3, inverses.at[1 - k])
    from_peer(4, crosses.at[1 - k])
    for one in peer_copies:
        one.wait_send()
    sent(pan_recv.at[pl.ds(0, 15)], pan_sems)
    sent(pb.at[0, 0, pl.ds(0, 7)], pb_sems)
    sent(pb.at[0, 0], px_sems)
    sent(xy.at[0, pl.ds(0, 4)], xy_far)
    sent(xy.at[0, pl.ds(0, 5)], xy_near)
    sent(xy.at[0, pl.ds(0, 6)], xy_relay)
    sent(zg.at[pl.ds(0, 3)], zx_sems)
    sent(zg.at[pl.ds(0, 12)], zy_sems)
    sent(rng_recv.at[pl.ds(0, 7)], rng_sems)
    sent(crosses.at[0, pl.ds(0, 7)], c_sems)


def finish_kernel(trail, bases, inverses, crosses, chosen, factors, trail_out, basis_out, coeff_out, coeff, sems):
    copies = [pltpu.make_async_copy(trail.at[pl.ds(1024 * i, 1024)], trail_out.at[pl.ds(1024 * i, 1024)], sems.at[i]) for i in range(8)]
    copies.append(pltpu.make_async_copy(bases, basis_out, sems.at[8]))
    for one in copies:
        one.start()
    both = jnp.concatenate([unfold(crosses.at[0]), unfold(crosses.at[1])], axis=0)
    both = pair_apply(select_dot(both, chosen[...], NN), factors) * (512.0**-0.5)
    for a in range(2):
        coeff[a] = dot(inverses[a][:, :64], both[64 * a : 64 * a + 64])
    copies.append(pltpu.make_async_copy(coeff, coeff_out, sems.at[9]))
    copies[9].start()
    for one in copies:
        one.wait()


def body(n_row, trail, panel, row_basis, row_coeff, col_basis, col_scaled, pivot_basis, pivot_scaled, sketch, perm, pair_kind, pivot_values):
    turn = lambda x: jnp.swapaxes(x[:, 0], 1, 2)
    dma = pltpu.SemaphoreType.DMA
    inputs = (
        turn(panel),
        turn(row_basis),
        turn(row_coeff),
        pivot_basis.T,
        turn(col_basis),
        turn(col_scaled),
        sketch,
        perm.reshape(1, 512),
        pair_kind.reshape(1, 256),
        pivot_values,
        pivot_scaled,
    )
    small = jax.ShapeDtypeStruct((2, 64, 512), F32)
    results = pl.pallas_call(
        functools.partial(panel_kernel, n_row),
        out_shape=(
            jax.ShapeDtypeStruct((8192, 128), F32),
            small,
            jax.ShapeDtypeStruct((2, 64, 128), F32),
            jax.ShapeDtypeStruct((2, 8, 32, 128), F32),
            jax.ShapeDtypeStruct((512, 512), BF16),
            jax.ShapeDtypeStruct((8, 512), F32),
        ),
        in_specs=[HBM] * 12,
        out_specs=(VMEM,) * 6,
        scratch_shapes=[
            pltpu.VMEM((2, 16, 32, 128), F32),
            pltpu.VMEM((2, 2, 8, 8, 128), F32),
            pltpu.VMEM((n_row, 2, 32, 128), F32),
            [pltpu.VMEM(x.shape, x.dtype) for x in inputs],
            pltpu.VMEM((2, 8, 16, 128), F32),
            pltpu.VMEM((16, 16, 128), F32),
            pltpu.VMEM((2, 32, 512), F32),
            pltpu.VMEM((512, 128), F32),
            pltpu.VMEM((2, 32, 128), F32),
            pltpu.VMEM((2, 8, 128), F32),
            pltpu.VMEM((2, 32, 128), F32),
            pltpu.VMEM((32, 128), F32),
            pltpu.VMEM((8, 32, 128), F32),
            pltpu.VMEM((32, 128), F32),
            pltpu.VMEM((512, 128), F32),
            pltpu.VMEM((64, 512), BF16),
            pltpu.VMEM((64, 512), BF16),
            pltpu.VMEM((64, 512), F32),
            *[dma((2,))] * 10,
            dma((6,)),
            dma((6,)),
            dma((11,)),
            dma(()),
            pltpu.VMEM((2, 2, 512, 256), BF16),
            pltpu.VMEM((2, 512, 256), BF16),
        ],
        compiler_params=pltpu.CompilerParams(
            collective_id=0, has_side_effects=True, vmem_limit_bytes=40 * 1024 * 1024
        ),
        name="panel",
    )(*[pltpu.with_memory_space_constraint(x, pltpu.HBM) for x in (trail.reshape(8192, 128), *inputs)])
    trail_out, basis_out, coeff_out = pl.pallas_call(
        finish_kernel,
        out_shape=(jax.ShapeDtypeStruct((8192, 128), F32), small, small),
        in_specs=[VMEM] * 6,
        out_specs=(HBM,) * 3,
        scratch_shapes=[pltpu.VMEM((2, 64, 512), F32), dma((10,))],
        compiler_params=pltpu.CompilerParams(vmem_limit_bytes=40 * 1024 * 1024),
        name="finish",
    )(*results)
    return (trail_out.reshape(trail.shape), basis_out[:, None], coeff_out[:, None])


def solution(mesh):
    n_row = mesh.shape["row"]
    return jax.shard_map(
        functools.partial(body, n_row),
        mesh=mesh,
        in_specs=(
            P(None, "row", None, None, "col", None),
            P(None, "row", None, "col"),
            P(None, "row", None, "col"),
            P(None, "row", None, "col"),
            P(None, "col", None, "row"),
            P(None, "col", None, "row"),
            P(None, "col"),
            P(),
            P(),
            P(),
            P(),
            P(),
        ),
        out_specs=(
            P(None, "row", None, None, "col", None),
            P(None, "row", None, None),
            P(None, "row", None, None),
        ),
        check_vma=False,
    )
```

```python
import functools

import jax
import jax.numpy as jnp
from jax import lax
from jax.experimental import pallas as pl
from jax.experimental.pallas import tpu as pltpu
from jax.sharding import PartitionSpec as P

MESH = pl.DeviceIdType.MESH
F32 = jnp.float32
BF16 = jnp.bfloat16
HIGHEST = lax.Precision.HIGHEST
NN = (((1,), (0,)), ((), ()))
NT = (((1,), (1,)), ((), ()))
TN = (((0,), (0,)), ((), ()))
VMEM = pl.BlockSpec(memory_space=pltpu.VMEM)
HBM = pl.BlockSpec(memory_space=pltpu.HBM)


def dot(a, b, dims=NN):
    return lax.dot_general(a, b, dims, precision=HIGHEST, preferred_element_type=F32)


def split3(x):
    high = x.astype(BF16)
    rest = x - high.astype(F32)
    mid = rest.astype(BF16)
    low = (rest - mid.astype(F32)).astype(BF16)
    return jnp.concatenate([high, mid, low], axis=0)


def split2(x):
    high = x.astype(BF16)
    return high, (x - high.astype(F32)).astype(BF16)


def bdot(a, b, dims=NN):
    return lax.dot_general(a, b, dims, preferred_element_type=F32)


def select_dot(x, chosen, dims):
    n = x.shape[0]
    out = lax.dot_general(split3(x), chosen, dims, preferred_element_type=F32)
    return (out[2 * n :] + out[n : 2 * n]) + out[:n]


def lower_half(shape):
    return lax.broadcasted_iota(jnp.int32, shape, 1) % 128 < 64


def swap(x):
    return pltpu.roll(x, 64, 1)


def fold(x):
    return jnp.where(lower_half((32, 128)), x[:32], swap(x[32:]))


def unfold(ref):
    low = lower_half((32, 128))
    tops, bottoms = [], []
    for j in range(4):
        even, odd = ref[2 * j], ref[2 * j + 1]
        tops.append(jnp.where(low, even, swap(odd)))
        bottoms.append(jnp.where(low, swap(even), odd))
    return jnp.concatenate([jnp.concatenate(tops, axis=1), jnp.concatenate(bottoms, axis=1)], axis=0)


def pair_apply(x, factors):
    odd = lax.broadcasted_iota(jnp.int32, x.shape, 1) % 2 == 1
    partner = jnp.where(odd, pltpu.roll(x, 1, 1), pltpu.roll(x, 511, 1))
    return x * factors[0:1] + partner * factors[1:2]


def inverse_factor(gram):
    rows = lax.broadcasted_iota(jnp.int32, (64, 64), 0)
    eye = (rows == lax.broadcasted_iota(jnp.int32, (64, 64), 1)).astype(F32)
    both = jnp.concatenate([gram, eye], axis=1)
    work = [both[8 * g : 8 * g + 8] for g in range(8)]
    sub = lax.broadcasted_iota(jnp.int32, (8, 128), 0)
    for k in range(8):
        columns = {
            (g, j): jnp.broadcast_to(work[g][:, 8 * k + j : 8 * k + j + 1], (8, 128))
            for g in range(k, 8)
            for j in range(8)
        }
        pivots = jnp.ones((8, 128), F32)
        for j in range(8):
            pivot = jnp.broadcast_to(columns[k, j][j : j + 1], (8, 128))
            pivots = jnp.where(sub == j, pivot, pivots)
            inverse = 1.0 / pivot
            scaled = jnp.broadcast_to(work[k][j : j + 1], (8, 128)) * inverse
            heads = {
                later: jnp.broadcast_to(columns[k, later][j : j + 1], (8, 128)) * inverse
                for later in range(j + 1, 8)
            }
            for g in range(k, 8):
                factor = columns[g, j]
                if g == k:
                    if j == 7:
                        continue
                    factor = jnp.where(sub > j, factor, 0.0)
                work[g] = work[g] - factor * scaled
                for later in range(j + 1, 8):
                    columns[g, later] = columns[g, later] - factor * heads[later]
        work[k] = work[k] * lax.rsqrt(pivots)
    return jnp.concatenate(work, axis=0)


def panel_kernel(
    n_row,
    trail_hbm,
    *refs,
):
    inputs, refs = refs[:11], refs[11:]
    run_panel(n_row, trail_hbm, inputs, *refs)


def run_panel(
    n_row,
    trail_hbm,
    inputs,
    trail,
    bases,
    inverses,
    crosses,
    chosen,
    factors,
    xy,
    pb,
    zg,
    staged,
    pan_send,
    pan_recv,
    pan_chip,
    pan_full,
    xy_send,
    pb_send,
    zg_send,
    rng_send,
    rng_recv,
    c_send,
    basis_full,
    panel_high,
    panel_low,
    ranges,
    pan_sems,
    pb_sems,
    px_sems,
    xy_far,
    xy_near,
    xy_relay,
    zx_sems,
    zy_sems,
    rng_sems,
    c_sems,
    hand_sems,
    peer_ss,
    peer_rs,
    in_sem,
    trail_sem,
    lefts,
    rights,
):
    r = lax.axis_index("row")
    c = lax.axis_index("col")
    z = c // 2
    k = c % 2
    peer = 2 * z + 1 - k

    y, x = r // 4, r % 4
    order = [8, 9, 7, 10, 6, 11, 5, 12, 4, 13, 3, 14, 2, 15, 1]

    steps = [4, 5, 3, 6, 2, 7, 1]

    barrier = pltpu.get_barrier_semaphore()
    for d in order:
        pl.semaphore_signal(barrier, inc=1, device_id=(r, (c + d) % 16), device_id_type=MESH)
    for d in (2, 1, 3):
        pl.semaphore_signal(barrier, inc=1, device_id=(4 * y + (x + d) % 4, c), device_id_type=MESH)
        pl.semaphore_signal(barrier, inc=1, device_id=(4 * ((y + d) % 4) + x, c), device_id_type=MESH)
    loads = [pltpu.make_async_copy(src, dst, in_sem.at[i]) for i, (src, dst) in enumerate(zip(inputs, staged))]
    for one in loads:
        one.start()
    trail_load = pltpu.make_async_copy(trail_hbm, trail, trail_sem)
    panel, row_basis, row_coeff, pivot_basis, col_basis, col_scaled, sketch, perm, pair_kind, pivot_values, pivot_scaled = staged

    for one in loads:
        one.wait()
    low16 = lower_half((16, 128))
    for a in range(2):
        for j in range(4):
            tile = panel[a, :, 128 * j : 128 * j + 128]
            top, bottom = tile[:16], tile[16:]
            pan_send[a, 2 * j] = jnp.where(low16, top, swap(bottom))
            pan_send[a, 2 * j + 1] = jnp.where(low16, swap(top), bottom)
        xy_send[a, :, :64] = row_basis[a]
        xy_send[a, :, 64:] = row_coeff[a]
        pb_send[a, :, :64] = pivot_basis[16 * a : 16 * a + 8]
        pb_send[a, :, 64:] = pivot_basis[16 * a + 8 : 16 * a + 16]
        zg_send[a, :, :64] = col_basis[a]
        zg_send[a, :, 64:] = col_scaled[a]
    pan_recv[c] = pan_send[k, z]
    xy[k, c] = xy_send[k]
    pb[k, x % 2, z] = pb_send[x % 2]
    zg[r] = zg_send[...]
    pan_chip[k] = panel[k]

    pl.semaphore_wait(barrier, 21)

    def copy(src, dst, send_sem, recv_sem, row, col):
        return pltpu.make_async_remote_copy(
            src_ref=src,
            dst_ref=dst,
            send_sem=send_sem,
            recv_sem=recv_sem,
            device_id=(row, col),
            device_id_type=MESH,
        )

    def send(src, dst, sems, row, col):
        copy(src, dst, sems.at[0], sems.at[1], row, col).start()

    def landed(ref, sems):
        copy(ref, ref, sems.at[0], sems.at[1], r, peer).wait_recv()

    def sent(ref, sems):
        copy(ref, ref, sems.at[0], sems.at[1], r, peer).wait_send()

    peer_copies = []

    def to_peer(i, src, dst):
        one = copy(src, dst, peer_ss.at[i], peer_rs.at[i], r, peer)
        one.start()
        peer_copies.append(one)

    def from_peer(i, ref):
        copy(ref, ref, peer_ss.at[i], peer_rs.at[i], r, peer).wait_recv()

    for d in order:
        to = (c + d) % 16
        send(pan_send.at[to % 2, to // 2], pan_recv.at[c], pan_sems, r, to)
    for d in (2, 1, 3):
        send(zg_send, zg.at[r], zx_sems, 4 * y + (x + d) % 4, c)
    for d in steps:
        send(pb_send.at[x % 2], pb.at[k, x % 2, z], pb_sems, r, 2 * ((z + d) % 8) + k)
    to_peer(0, panel.at[1 - k], pan_chip.at[k])
    for d in (2, 6, 1, 7):
        for core in range(2):
            to = 2 * ((z + d) % 8) + core
            send(xy_send.at[core], xy.at[core, c], xy_far if d in (2, 6) else xy_near, r, to)
    send(xy_send.at[1 - k], xy.at[1 - k, c], xy_near, r, peer)

    trail_load.start()
    q_ids = lax.broadcasted_iota(jnp.int32, (512, 512), 0)
    chosen[...] = (q_ids == perm[...]).astype(F32).astype(BF16)
    t_ids = lax.broadcasted_iota(jnp.int32, (256, 512), 1)
    spread = (t_ids // 2 == lax.broadcasted_iota(jnp.int32, (256, 512), 0)).astype(F32).astype(BF16)
    values = jnp.concatenate([pivot_values[...], pair_kind[...].astype(F32), jnp.zeros((4, 256), F32)], axis=0)
    values = select_dot(values, spread, NN)
    first, second, offdiag, twin = values[0:1], values[1:2], values[2:3], values[3:4] > 0.5
    odd = lax.broadcasted_iota(jnp.int32, (1, 512), 1) % 2 == 1
    own = jnp.where(odd, second, first)
    other = jnp.where(odd, first, second)
    determinant = first * second - offdiag * offdiag
    alpha = jnp.where(twin, other / determinant, 1.0 / own)
    beta = jnp.where(twin, -offdiag / determinant, 0.0)

    factors[...] = jnp.concatenate([alpha, beta, jnp.zeros((6, 512), F32)], axis=0)
    scaled = select_dot(pair_apply(sketch[...], factors), chosen[...], NT)

    mine = pl.ds(pl.multiple_of(4 * y, 4), 4)
    landed(zg.at[pl.ds(0, 3)], zx_sems)
    for d in (2, 1, 3):
        send(zg.at[mine], zg.at[mine], zy_sems, 4 * ((y + d) % 4) + x, c)
    landed(pan_recv.at[pl.ds(0, 15)], pan_sems)
    for i in range(16):
        block = pan_recv[i]
        pan_full[32 * i : 32 * i + 16] = block
        pan_full[32 * i + 16 : 32 * i + 32] = swap(block)
    folded = fold(dot(scaled, pan_full[...]))
    rng_send[...] = folded
    rng_recv[z] = folded
    for d in steps:
        to = 2 * ((z + d) % 8) + k
        send(rng_send, rng_recv.at[z], rng_sems, r, to)

    landed(pb.at[0, 0, pl.ds(0, 7)], pb_sems)
    send(pb.at[k, x % 2], pb.at[k, x % 2], px_sems, 4 * y + x + 1 - 2 * (x % 2), c)
    landed(xy.at[0, pl.ds(0, 4)], xy_far)
    for d, side in ((6, 1), (2, -1)):
        origin = 2 * ((z + d) % 8)
        both = xy.at[k, pl.ds(pl.multiple_of(origin, 2), 2)]
        send(both, both, xy_relay, r, 2 * ((z + side) % 8) + k)
        one = xy.at[k, origin + (d == 2)]
        send(one, one, xy_relay, r, 2 * ((z + 2 * side) % 8) + k)
    landed(pb.at[0, 0], px_sems)
    to_peer(5, pb.at[k], pb.at[k])
    from_peer(0, pan_chip.at[1 - k])
    from_peer(5, pb.at[1 - k])
    for i in range(16):
        for half in range(2):
            block = pb[i % 2, half, i // 2]
            at = 32 * i + 16 * half
            basis_full[at : at + 8] = block
            basis_full[at + 8 : at + 16] = swap(block)
    weights = dot(scaled, basis_full[...])[:, :64]
    mine = basis_full[pl.ds(pl.multiple_of(64 * z, 64), 64), :][:, :64]
    mixer = dot(jnp.concatenate([weights, mine], axis=0), pivot_scaled[...])
    mixer_high, mixer_low = split2(mixer)
    mixer_both = jnp.concatenate([mixer_high, mixer_low], axis=0)
    landed(xy.at[0, pl.ds(0, 5)], xy_near)
    landed(xy.at[0, pl.ds(0, 6)], xy_relay)
    to_peer(1, xy.at[k], xy.at[k])
    left_high, left_low = split2(xy[k].reshape(512, 128))
    mixed = bdot(mixer_both, left_high)
    mixed = (bdot(mixer_high, left_low) + mixed[128:]) + mixed[:128]
    mixed = jnp.where(lower_half((128, 128)), swap(mixed), 0.0)
    mixed_high, mixed_low = split2(mixed)
    fixes = bdot(mixed_high, left_low, NT) + bdot(
        jnp.concatenate([mixed_high, mixed_low], axis=1), jnp.concatenate([left_high, left_high], axis=1), NT
    )
    panel_high[...], panel_low[...] = split2(pan_chip[...].reshape(64, 512) - fixes[64:])

    landed(rng_recv.at[pl.ds(0, 7)], rng_sems)
    total = unfold(rng_recv) - fixes[:64]
    ranges[...] = total
    total_high, total_low = split2(total)
    cross = bdot(jnp.concatenate([total_high, total_low], axis=0), panel_high[...], NT)
    cross = (bdot(total_high, panel_low[...], NT) + cross[64:]) + cross[:64]
    cross = jnp.concatenate([cross, cross], axis=1)
    folded = jnp.where(lower_half((32, 128)), cross[:32], cross[32:])
    c_send[...] = folded

    def cross_copy(to):
        return copy(c_send, crosses.at[k, z], c_sems.at[0], c_sems.at[1 + k], r, to)

    for d in steps:
        cross_copy(2 * ((z + d) % 8) + 1).start()

    @pl.when(k == 0)
    def _():
        cross_copy(peer).start()

    @pl.when(k == 1)
    def _():
        crosses[1, z] = folded

    @pl.when(c < 16)
    def _():
        total = ranges[...]
        inverse = swap(inverse_factor(dot(total, total, NT) * (1.0 / 512.0)))
        inverses[k] = inverse
        bases[k] = dot(inverse[:, :64], total)

    to_peer(2, bases.at[k], bases.at[k])
    to_peer(3, inverses.at[k], inverses.at[k])
    from_peer(1, xy.at[1 - k])
    landed(zg.at[pl.ds(0, 12)], zy_sems)
    trail_load.wait()
    low = lower_half((512, 128))
    columns = []
    for b in range(2):
        both = zg[:, b].reshape(512, 128)
        columns.append(both)
        twice = jnp.where(low, both, swap(both))
        high = twice.astype(BF16).astype(F32)
        pair = jnp.where(low, high, twice - high).astype(BF16)
        rights[b] = jnp.concatenate([pair, pair], axis=1)
    columns_high, columns_low = split2(jnp.concatenate(columns, axis=1))
    rows_high, rows_low = split2(jnp.concatenate([xy[0].reshape(512, 128), xy[1].reshape(512, 128)], axis=1))
    cores = bdot(rows_high, columns_low, TN) + bdot(rows_low, columns_high, TN) + bdot(rows_high, columns_high, TN)
    low = lower_half((64, 128))
    for a in range(2):
        core = cores[128 * a + 64 : 128 * a + 128]
        core = [jnp.where(low, swap(half), half) for half in (core[:, :128], core[:, 128:])]
        core = jnp.concatenate([jnp.concatenate(core, axis=1), jnp.zeros((64, 256), F32)], axis=0)
        core_high, core_low = split2(core)
        high, rest = rows_high[:, 128 * a : 128 * a + 128], rows_low[:, 128 * a : 128 * a + 128]
        left = bdot(high, core_low) + bdot(
            jnp.concatenate([high, rest], axis=1), jnp.concatenate([core_high, core_high], axis=0)
        )
        high, rest = split2(left)
        for b in range(2):
            lefts[a, b, :, :128] = high[:, 128 * b : 128 * b + 128]
            lefts[a, b, :, 128:] = rest[:, 128 * b : 128 * b + 128]

    def change(a, parts):
        @pl.when(c < 16)
        def _():
            for part in parts:
                for b in range(2):
                    delta = bdot(lefts[a, b, 128 * part : 128 * part + 128], rights[b], NT)
                    for j in range(4):
                        lines = pl.ds(4096 * a + 1024 * part + 4 * b + j, 128, stride=8)
                        trail[lines, :] = trail[lines, :] - delta[:, 128 * j : 128 * j + 128]

    change(0, range(4))

    def hand_over(a, count):
        block = crosses.at[a, pl.ds(0, count)]
        copy(block, block, c_sems.at[0], c_sems.at[1 + a], r, peer).wait_recv()
        copy(crosses.at[a], crosses.at[a], hand_sems.at[a], hand_sems.at[2 + a], r, peer).start()

    @pl.when(k == 1)
    def _():
        hand_over(1, 7)
        hand_over(0, 8)

    change(1, range(4))
    from_peer(2, bases.at[1 - k])
    from_peer(3, inverses.at[1 - k])

    @pl.when(k == 0)
    def _():
        for a in (1, 0):
            copy(crosses.at[a], crosses.at[a], hand_sems.at[a], hand_sems.at[2 + a], r, peer).wait_recv()

    for one in peer_copies:
        one.wait_send()
    sent(pan_recv.at[pl.ds(0, 15)], pan_sems)
    sent(pb.at[0, 0, pl.ds(0, 7)], pb_sems)
    sent(pb.at[0, 0], px_sems)
    sent(xy.at[0, pl.ds(0, 4)], xy_far)
    sent(xy.at[0, pl.ds(0, 5)], xy_near)
    sent(xy.at[0, pl.ds(0, 6)], xy_relay)
    sent(zg.at[pl.ds(0, 3)], zx_sems)
    sent(zg.at[pl.ds(0, 12)], zy_sems)
    sent(rng_recv.at[pl.ds(0, 7)], rng_sems)
    copy(crosses.at[0, pl.ds(0, 7)], crosses.at[0, pl.ds(0, 7)], c_sems.at[0], c_sems.at[1], r, peer).wait_send()

    @pl.when(k == 0)
    def _():
        cross_copy(peer).wait_send()

    @pl.when(k == 1)
    def _():
        for a in (1, 0):
            copy(crosses.at[a], crosses.at[a], hand_sems.at[a], hand_sems.at[2 + a], r, peer).wait_send()


def finish_kernel(trail, bases, inverses, crosses, chosen, factors, trail_out, basis_out, coeff_out, coeff, sems):
    copies = [pltpu.make_async_copy(trail.at[pl.ds(2048 * i, 2048)], trail_out.at[pl.ds(2048 * i, 2048)], sems.at[i]) for i in range(4)]
    copies.append(pltpu.make_async_copy(bases, basis_out, sems.at[4]))
    for one in copies:
        one.start()
    both = jnp.concatenate([unfold(crosses.at[0]), unfold(crosses.at[1])], axis=0)
    both = pair_apply(select_dot(both, chosen[...], NN), factors) * (512.0**-0.5)
    for a in range(2):
        coeff[a] = dot(inverses[a][:, :64], both[64 * a : 64 * a + 64])
    copies.append(pltpu.make_async_copy(coeff, coeff_out, sems.at[5]))
    copies[5].start()
    for one in copies:
        one.wait()


def body(n_row, trail, panel, row_basis, row_coeff, col_basis, col_scaled, pivot_basis, pivot_scaled, sketch, perm, pair_kind, pivot_values):
    turn = lambda x: jnp.swapaxes(x[:, 0], 1, 2)
    dma = pltpu.SemaphoreType.DMA
    inputs = (
        turn(panel),
        turn(row_basis),
        turn(row_coeff),
        pivot_basis.T,
        turn(col_basis),
        turn(col_scaled),
        sketch,
        perm.reshape(1, 512),
        pair_kind.reshape(1, 256),
        pivot_values,
        pivot_scaled,
    )
    small = jax.ShapeDtypeStruct((2, 64, 512), F32)
    results = pl.pallas_call(
        functools.partial(panel_kernel, n_row),
        out_shape=(
            jax.ShapeDtypeStruct((8192, 128), F32),
            small,
            jax.ShapeDtypeStruct((2, 64, 128), F32),
            jax.ShapeDtypeStruct((2, 8, 32, 128), F32),
            jax.ShapeDtypeStruct((512, 512), BF16),
            jax.ShapeDtypeStruct((8, 512), F32),
        ),
        in_specs=[HBM] * 12,
        out_specs=(VMEM,) * 6,
        scratch_shapes=[
            pltpu.VMEM((2, 16, 32, 128), F32),
            pltpu.VMEM((2, 2, 8, 8, 128), F32),
            pltpu.VMEM((n_row, 2, 32, 128), F32),
            [pltpu.VMEM(x.shape, x.dtype) for x in inputs],
            pltpu.VMEM((2, 8, 16, 128), F32),
            pltpu.VMEM((16, 16, 128), F32),
            pltpu.VMEM((2, 32, 512), F32),
            pltpu.VMEM((512, 128), F32),
            pltpu.VMEM((2, 32, 128), F32),
            pltpu.VMEM((2, 8, 128), F32),
            pltpu.VMEM((2, 32, 128), F32),
            pltpu.VMEM((32, 128), F32),
            pltpu.VMEM((8, 32, 128), F32),
            pltpu.VMEM((32, 128), F32),
            pltpu.VMEM((512, 128), F32),
            pltpu.VMEM((64, 512), BF16),
            pltpu.VMEM((64, 512), BF16),
            pltpu.VMEM((64, 512), F32),
            *[dma((2,))] * 9,
            dma((3,)),
            dma((4,)),
            dma((6,)),
            dma((6,)),
            dma((11,)),
            dma(()),
            pltpu.VMEM((2, 2, 512, 256), BF16),
            pltpu.VMEM((2, 512, 256), BF16),
        ],
        compiler_params=pltpu.CompilerParams(
            collective_id=0, has_side_effects=True, vmem_limit_bytes=40 * 1024 * 1024
        ),
        name="panel",
    )(*[pltpu.with_memory_space_constraint(x, pltpu.HBM) for x in (trail.reshape(8192, 128), *inputs)])
    trail_out, basis_out, coeff_out = pl.pallas_call(
        finish_kernel,
        out_shape=(jax.ShapeDtypeStruct((8192, 128), F32), small, small),
        in_specs=[VMEM] * 6,
        out_specs=(HBM,) * 3,
        scratch_shapes=[pltpu.VMEM((2, 64, 512), F32), dma((6,))],
        compiler_params=pltpu.CompilerParams(vmem_limit_bytes=40 * 1024 * 1024),
        name="finish",
    )(*results)
    return (trail_out.reshape(trail.shape), basis_out[:, None], coeff_out[:, None])


def solution(mesh):
    n_row = mesh.shape["row"]
    return jax.shard_map(
        functools.partial(body, n_row),
        mesh=mesh,
        in_specs=(
            P(None, "row", None, None, "col", None),
            P(None, "row", None, "col"),
            P(None, "row", None, "col"),
            P(None, "row", None, "col"),
            P(None, "col", None, "row"),
            P(None, "col", None, "row"),
            P(None, "col"),
            P(),
            P(),
            P(),
            P(),
            P(),
        ),
        out_specs=(
            P(None, "row", None, None, "col", None),
            P(None, "row", None, None),
            P(None, "row", None, None),
        ),
        check_vma=False,
    )
```

```python
import functools

import jax
import jax.numpy as jnp
from jax import lax
from jax.experimental import pallas as pl
from jax.experimental.pallas import tpu as pltpu
from jax.sharding import PartitionSpec as P

MESH = pl.DeviceIdType.MESH
F32 = jnp.float32
BF16 = jnp.bfloat16
HIGHEST = lax.Precision.HIGHEST
NN = (((1,), (0,)), ((), ()))
NT = (((1,), (1,)), ((), ()))
TN = (((0,), (0,)), ((), ()))
VMEM = pl.BlockSpec(memory_space=pltpu.VMEM)
HBM = pl.BlockSpec(memory_space=pltpu.HBM)


def dot(a, b, dims=NN):
    return lax.dot_general(a, b, dims, precision=HIGHEST, preferred_element_type=F32)


def split3(x):
    high = x.astype(BF16)
    rest = x - high.astype(F32)
    mid = rest.astype(BF16)
    low = (rest - mid.astype(F32)).astype(BF16)
    return jnp.concatenate([high, mid, low], axis=0)


def split2(x):
    high = x.astype(BF16)
    return high, (x - high.astype(F32)).astype(BF16)


def bdot(a, b, dims=NN):
    return lax.dot_general(a, b, dims, preferred_element_type=F32)


def select_dot(x, chosen, dims):
    n = x.shape[0]
    out = lax.dot_general(split3(x), chosen, dims, preferred_element_type=F32)
    return (out[2 * n :] + out[n : 2 * n]) + out[:n]


def lower_half(shape):
    return lax.broadcasted_iota(jnp.int32, shape, 1) % 128 < 64


def swap(x):
    return pltpu.roll(x, 64, 1)


def fold(x):
    return jnp.where(lower_half((32, 128)), x[:32], swap(x[32:]))


def unfold(ref):
    low = lower_half((32, 128))
    tops, bottoms = [], []
    for j in range(4):
        even, odd = ref[2 * j], ref[2 * j + 1]
        tops.append(jnp.where(low, even, swap(odd)))
        bottoms.append(jnp.where(low, swap(even), odd))
    return jnp.concatenate([jnp.concatenate(tops, axis=1), jnp.concatenate(bottoms, axis=1)], axis=0)


def pair_apply(x, factors):
    odd = lax.broadcasted_iota(jnp.int32, x.shape, 1) % 2 == 1
    partner = jnp.where(odd, pltpu.roll(x, 1, 1), pltpu.roll(x, 511, 1))
    return x * factors[0:1] + partner * factors[1:2]


def inverse_factor(gram):
    rows = lax.broadcasted_iota(jnp.int32, (64, 64), 0)
    eye = (rows == lax.broadcasted_iota(jnp.int32, (64, 64), 1)).astype(F32)
    both = jnp.concatenate([gram, eye], axis=1)
    work = [both[8 * g : 8 * g + 8] for g in range(8)]
    sub = lax.broadcasted_iota(jnp.int32, (8, 128), 0)
    for k in range(8):
        columns = {
            (g, j): jnp.broadcast_to(work[g][:, 8 * k + j : 8 * k + j + 1], (8, 128))
            for g in range(k, 8)
            for j in range(8)
        }
        pivots = jnp.ones((8, 128), F32)
        for j in range(8):
            pivot = jnp.broadcast_to(columns[k, j][j : j + 1], (8, 128))
            pivots = jnp.where(sub == j, pivot, pivots)
            inverse = 1.0 / pivot
            scaled = jnp.broadcast_to(work[k][j : j + 1], (8, 128)) * inverse
            heads = {
                later: jnp.broadcast_to(columns[k, later][j : j + 1], (8, 128)) * inverse
                for later in range(j + 1, 8)
            }
            for g in range(k, 8):
                factor = columns[g, j]
                if g == k:
                    if j == 7:
                        continue
                    factor = jnp.where(sub > j, factor, 0.0)
                work[g] = work[g] - factor * scaled
                for later in range(j + 1, 8):
                    columns[g, later] = columns[g, later] - factor * heads[later]
        work[k] = work[k] * lax.rsqrt(pivots)
    return jnp.concatenate(work, axis=0)


def panel_kernel(
    n_row,
    trail_hbm,
    *refs,
):
    inputs, refs = refs[:11], refs[11:]
    run_panel(n_row, trail_hbm, inputs, *refs)


def run_panel(
    n_row,
    trail_hbm,
    inputs,
    trail,
    bases,
    inverses,
    crosses,
    chosen,
    factors,
    xy,
    pb,
    zg,
    staged,
    pan_send,
    pan_recv,
    pan_chip,
    pan_full,
    xy_send,
    pb_send,
    zg_send,
    rng_send,
    rng_recv,
    c_send,
    basis_full,
    panel_high,
    panel_low,
    ranges,
    pan_sems,
    pb_sems,
    px_sems,
    xy_far,
    xy_near,
    xy_relay,
    zx_sems,
    zy_sems,
    rng_sems,
    c_sems,
    hand_sems,
    out_sem,
    peer_rs,
    in_sem,
    trail_sem,
    lefts,
    rights,
):
    r = lax.axis_index("row")
    c = lax.axis_index("col")
    z = c // 2
    k = c % 2
    peer = 2 * z + 1 - k

    y, x = r // 4, r % 4
    order = [8, 9, 7, 10, 6, 11, 5, 12, 4, 13, 3, 14, 2, 15, 1]

    steps = [4, 5, 3, 6, 2, 7, 1]

    barrier = pltpu.get_barrier_semaphore()
    for d in order:
        pl.semaphore_signal(barrier, inc=1, device_id=(r, (c + d) % 16), device_id_type=MESH)
    for d in (2, 1, 3):
        pl.semaphore_signal(barrier, inc=1, device_id=(4 * y + (x + d) % 4, c), device_id_type=MESH)
        pl.semaphore_signal(barrier, inc=1, device_id=(4 * ((y + d) % 4) + x, c), device_id_type=MESH)
    loads = [pltpu.make_async_copy(src, dst, in_sem.at[i]) for i, (src, dst) in enumerate(zip(inputs, staged))]
    for one in loads:
        one.start()
    trail_load = pltpu.make_async_copy(trail_hbm, trail, trail_sem)
    panel, row_basis, row_coeff, pivot_basis, col_basis, col_scaled, sketch, perm, pair_kind, pivot_values, pivot_scaled = staged

    for one in loads:
        one.wait()
    low16 = lower_half((16, 128))
    for a in range(2):
        for j in range(4):
            tile = panel[a, :, 128 * j : 128 * j + 128]
            top, bottom = tile[:16], tile[16:]
            pan_send[a, 2 * j] = jnp.where(low16, top, swap(bottom))
            pan_send[a, 2 * j + 1] = jnp.where(low16, swap(top), bottom)
        xy_send[a, :, :64] = row_basis[a]
        xy_send[a, :, 64:] = row_coeff[a]
        pb_send[a, :, :64] = pivot_basis[16 * a : 16 * a + 8]
        pb_send[a, :, 64:] = pivot_basis[16 * a + 8 : 16 * a + 16]
        zg_send[a, :, :64] = col_basis[a]
        zg_send[a, :, 64:] = col_scaled[a]
    pan_recv[c] = pan_send[k, z]
    xy[k, c] = xy_send[k]
    pb[k, x % 2, z] = pb_send[x % 2]
    zg[r] = zg_send[...]
    pan_chip[k] = panel[k]

    pl.semaphore_wait(barrier, 21)

    def copy(src, dst, send_sem, recv_sem, row, col):
        return pltpu.make_async_remote_copy(
            src_ref=src,
            dst_ref=dst,
            send_sem=send_sem,
            recv_sem=recv_sem,
            device_id=(row, col),
            device_id_type=MESH,
        )

    def send(src, dst, sems, row, col):
        copy(src, dst, out_sem, sems.at[0], row, col).start()

    def landed(ref, sems):
        copy(ref, ref, out_sem, sems.at[0], r, peer).wait_recv()

    def to_peer(i, src, dst):
        copy(src, dst, out_sem, peer_rs.at[i], r, peer).start()

    def from_peer(i, ref):
        copy(ref, ref, out_sem, peer_rs.at[i], r, peer).wait_recv()

    for d in order:
        to = (c + d) % 16
        send(pan_send.at[to % 2, to // 2], pan_recv.at[c], pan_sems, r, to)
    for d in (2, 1, 3):
        send(zg_send, zg.at[r], zx_sems, 4 * y + (x + d) % 4, c)
    for d in steps:
        send(pb_send.at[x % 2], pb.at[k, x % 2, z], pb_sems, r, 2 * ((z + d) % 8) + k)
    to_peer(0, panel.at[1 - k], pan_chip.at[k])
    for d in (2, 6, 1, 7):
        for core in range(2):
            to = 2 * ((z + d) % 8) + core
            send(xy_send.at[core], xy.at[core, c], xy_far if d in (2, 6) else xy_near, r, to)
    send(xy_send.at[1 - k], xy.at[1 - k, c], xy_near, r, peer)

    trail_load.start()
    q_ids = lax.broadcasted_iota(jnp.int32, (512, 512), 0)
    chosen[...] = (q_ids == perm[...]).astype(F32).astype(BF16)
    t_ids = lax.broadcasted_iota(jnp.int32, (256, 512), 1)
    spread = (t_ids // 2 == lax.broadcasted_iota(jnp.int32, (256, 512), 0)).astype(F32).astype(BF16)
    values = jnp.concatenate([pivot_values[...], pair_kind[...].astype(F32), jnp.zeros((4, 256), F32)], axis=0)
    values = select_dot(values, spread, NN)
    first, second, offdiag, twin = values[0:1], values[1:2], values[2:3], values[3:4] > 0.5
    odd = lax.broadcasted_iota(jnp.int32, (1, 512), 1) % 2 == 1
    own = jnp.where(odd, second, first)
    other = jnp.where(odd, first, second)
    determinant = first * second - offdiag * offdiag
    alpha = jnp.where(twin, other / determinant, 1.0 / own)
    beta = jnp.where(twin, -offdiag / determinant, 0.0)

    factors[...] = jnp.concatenate([alpha, beta, jnp.zeros((6, 512), F32)], axis=0)
    scaled = select_dot(pair_apply(sketch[...], factors), chosen[...], NT)

    mine = pl.ds(pl.multiple_of(4 * y, 4), 4)
    landed(zg.at[pl.ds(0, 3)], zx_sems)
    for d in (2, 1, 3):
        send(zg.at[mine], zg.at[mine], zy_sems, 4 * ((y + d) % 4) + x, c)
    landed(pan_recv.at[pl.ds(0, 15)], pan_sems)
    for i in range(16):
        block = pan_recv[i]
        pan_full[32 * i : 32 * i + 16] = block
        pan_full[32 * i + 16 : 32 * i + 32] = swap(block)
    folded = fold(dot(scaled, pan_full[...]))
    rng_send[...] = folded
    rng_recv[z] = folded
    for d in steps:
        to = 2 * ((z + d) % 8) + k
        send(rng_send, rng_recv.at[z], rng_sems, r, to)

    landed(pb.at[0, 0, pl.ds(0, 7)], pb_sems)
    send(pb.at[k, x % 2], pb.at[k, x % 2], px_sems, 4 * y + x + 1 - 2 * (x % 2), c)
    landed(xy.at[0, pl.ds(0, 4)], xy_far)
    for d, side in ((6, 1), (2, -1)):
        origin = 2 * ((z + d) % 8)
        both = xy.at[k, pl.ds(pl.multiple_of(origin, 2), 2)]
        send(both, both, xy_relay, r, 2 * ((z + side) % 8) + k)
        one = xy.at[k, origin + (d == 2)]
        send(one, one, xy_relay, r, 2 * ((z + 2 * side) % 8) + k)
    landed(pb.at[0, 0], px_sems)
    to_peer(5, pb.at[k], pb.at[k])
    from_peer(0, pan_chip.at[1 - k])
    from_peer(5, pb.at[1 - k])
    for i in range(16):
        for half in range(2):
            block = pb[i % 2, half, i // 2]
            at = 32 * i + 16 * half
            basis_full[at : at + 8] = block
            basis_full[at + 8 : at + 16] = swap(block)
    weights = dot(scaled, basis_full[...])[:, :64]
    mine = basis_full[pl.ds(pl.multiple_of(64 * z, 64), 64), :][:, :64]
    mixer = dot(jnp.concatenate([weights, mine], axis=0), pivot_scaled[...])
    mixer_high, mixer_low = split2(mixer)
    mixer_both = jnp.concatenate([mixer_high, mixer_low], axis=0)
    landed(xy.at[0, pl.ds(0, 5)], xy_near)
    landed(xy.at[0, pl.ds(0, 6)], xy_relay)
    to_peer(1, xy.at[k], xy.at[k])
    left_high, left_low = split2(xy[k].reshape(512, 128))
    mixed = bdot(mixer_both, left_high)
    mixed = (bdot(mixer_high, left_low) + mixed[128:]) + mixed[:128]
    mixed = jnp.where(lower_half((128, 128)), swap(mixed), 0.0)
    mixed_high, mixed_low = split2(mixed)
    fixes = bdot(mixed_high, left_low, NT) + bdot(
        jnp.concatenate([mixed_high, mixed_low], axis=1), jnp.concatenate([left_high, left_high], axis=1), NT
    )
    panel_high[...], panel_low[...] = split2(pan_chip[...].reshape(64, 512) - fixes[64:])

    landed(rng_recv.at[pl.ds(0, 7)], rng_sems)
    total = unfold(rng_recv) - fixes[:64]
    ranges[...] = total
    total_high, total_low = split2(total)
    cross = bdot(jnp.concatenate([total_high, total_low], axis=0), panel_high[...], NT)
    cross = (bdot(total_high, panel_low[...], NT) + cross[64:]) + cross[:64]
    cross = jnp.concatenate([cross, cross], axis=1)
    folded = jnp.where(lower_half((32, 128)), cross[:32], cross[32:])
    c_send[...] = folded

    def cross_copy(to):
        return copy(c_send, crosses.at[k, z], c_sems.at[0], c_sems.at[1 + k], r, to)

    for d in steps:
        cross_copy(2 * ((z + d) % 8) + 1).start()

    @pl.when(k == 0)
    def _():
        cross_copy(peer).start()

    @pl.when(k == 1)
    def _():
        crosses[1, z] = folded

    @pl.when(c < 16)
    def _():
        total = ranges[...]
        inverse = swap(inverse_factor(dot(total, total, NT) * (1.0 / 512.0)))
        inverses[k] = inverse
        bases[k] = dot(inverse[:, :64], total)

    to_peer(2, bases.at[k], bases.at[k])
    to_peer(3, inverses.at[k], inverses.at[k])
    from_peer(1, xy.at[1 - k])
    landed(zg.at[pl.ds(0, 12)], zy_sems)
    trail_load.wait()
    low = lower_half((512, 128))
    columns = []
    for b in range(2):
        both = zg[:, b].reshape(512, 128)
        columns.append(both)
        twice = jnp.where(low, both, swap(both))
        high = twice.astype(BF16).astype(F32)
        pair = jnp.where(low, high, twice - high).astype(BF16)
        rights[b] = jnp.concatenate([pair, pair], axis=1)
    columns_high, columns_low = split2(jnp.concatenate(columns, axis=1))
    rows_high, rows_low = split2(jnp.concatenate([xy[0].reshape(512, 128), xy[1].reshape(512, 128)], axis=1))
    cores = bdot(rows_high, columns_low, TN) + bdot(rows_low, columns_high, TN) + bdot(rows_high, columns_high, TN)
    low = lower_half((64, 128))
    for a in range(2):
        core = cores[128 * a + 64 : 128 * a + 128]
        core = [jnp.where(low, swap(half), half) for half in (core[:, :128], core[:, 128:])]
        core = jnp.concatenate([jnp.concatenate(core, axis=1), jnp.zeros((64, 256), F32)], axis=0)
        core_high, core_low = split2(core)
        high, rest = rows_high[:, 128 * a : 128 * a + 128], rows_low[:, 128 * a : 128 * a + 128]
        left = bdot(high, core_low) + bdot(
            jnp.concatenate([high, rest], axis=1), jnp.concatenate([core_high, core_high], axis=0)
        )
        high, rest = split2(left)
        for b in range(2):
            lefts[a, b, :, :128] = high[:, 128 * b : 128 * b + 128]
            lefts[a, b, :, 128:] = rest[:, 128 * b : 128 * b + 128]

    def change(a, parts):
        @pl.when(c < 16)
        def _():
            for part in parts:
                for b in range(2):
                    delta = bdot(lefts[a, b, 128 * part : 128 * part + 128], rights[b], NT)
                    for j in range(4):
                        lines = pl.ds(4096 * a + 1024 * part + 4 * b + j, 128, stride=8)
                        trail[lines, :] = trail[lines, :] - delta[:, 128 * j : 128 * j + 128]

    change(0, range(4))

    def hand_over(a, count):
        block = crosses.at[a, pl.ds(0, count)]
        copy(block, block, c_sems.at[0], c_sems.at[1 + a], r, peer).wait_recv()
        copy(crosses.at[a], crosses.at[a], hand_sems.at[a], hand_sems.at[2 + a], r, peer).start()

    @pl.when(k == 1)
    def _():
        hand_over(1, 7)
        hand_over(0, 8)

    change(1, range(4))
    from_peer(2, bases.at[1 - k])
    from_peer(3, inverses.at[1 - k])

    @pl.when(k == 0)
    def _():
        for a in (1, 0):
            copy(crosses.at[a], crosses.at[a], hand_sems.at[a], hand_sems.at[2 + a], r, peer).wait_recv()

    all_sent = trail.at[pl.ds(0, 2 * 1556)]
    copy(all_sent, all_sent, out_sem, c_sems.at[1], r, peer).wait_send()
    copy(crosses.at[0, pl.ds(0, 7)], crosses.at[0, pl.ds(0, 7)], c_sems.at[0], c_sems.at[1], r, peer).wait_send()

    @pl.when(k == 0)
    def _():
        cross_copy(peer).wait_send()

    @pl.when(k == 1)
    def _():
        for a in (1, 0):
            copy(crosses.at[a], crosses.at[a], hand_sems.at[a], hand_sems.at[2 + a], r, peer).wait_send()


def finish_kernel(trail, bases, inverses, crosses, chosen, factors, trail_out, basis_out, coeff_out, coeff, sems):
    copies = [pltpu.make_async_copy(trail.at[pl.ds(2048 * i, 2048)], trail_out.at[pl.ds(2048 * i, 2048)], sems.at[i]) for i in range(4)]
    copies.append(pltpu.make_async_copy(bases, basis_out, sems.at[4]))
    for one in copies:
        one.start()
    both = jnp.concatenate([unfold(crosses.at[0]), unfold(crosses.at[1])], axis=0)
    both = pair_apply(select_dot(both, chosen[...], NN), factors) * (512.0**-0.5)
    for a in range(2):
        coeff[a] = dot(inverses[a][:, :64], both[64 * a : 64 * a + 64])
    copies.append(pltpu.make_async_copy(coeff, coeff_out, sems.at[5]))
    copies[5].start()
    for one in copies:
        one.wait()


def body(n_row, trail, panel, row_basis, row_coeff, col_basis, col_scaled, pivot_basis, pivot_scaled, sketch, perm, pair_kind, pivot_values):
    turn = lambda x: jnp.swapaxes(x[:, 0], 1, 2)
    dma = pltpu.SemaphoreType.DMA
    inputs = (
        turn(panel),
        turn(row_basis),
        turn(row_coeff),
        pivot_basis.T,
        turn(col_basis),
        turn(col_scaled),
        sketch,
        perm.reshape(1, 512),
        pair_kind.reshape(1, 256),
        pivot_values,
        pivot_scaled,
    )
    small = jax.ShapeDtypeStruct((2, 64, 512), F32)
    results = pl.pallas_call(
        functools.partial(panel_kernel, n_row),
        out_shape=(
            jax.ShapeDtypeStruct((8192, 128), F32),
            small,
            jax.ShapeDtypeStruct((2, 64, 128), F32),
            jax.ShapeDtypeStruct((2, 8, 32, 128), F32),
            jax.ShapeDtypeStruct((512, 512), BF16),
            jax.ShapeDtypeStruct((8, 512), F32),
        ),
        in_specs=[HBM] * 12,
        out_specs=(VMEM,) * 6,
        scratch_shapes=[
            pltpu.VMEM((2, 16, 32, 128), F32),
            pltpu.VMEM((2, 2, 8, 8, 128), F32),
            pltpu.VMEM((n_row, 2, 32, 128), F32),
            [pltpu.VMEM(x.shape, x.dtype) for x in inputs],
            pltpu.VMEM((2, 8, 16, 128), F32),
            pltpu.VMEM((16, 16, 128), F32),
            pltpu.VMEM((2, 32, 512), F32),
            pltpu.VMEM((512, 128), F32),
            pltpu.VMEM((2, 32, 128), F32),
            pltpu.VMEM((2, 8, 128), F32),
            pltpu.VMEM((2, 32, 128), F32),
            pltpu.VMEM((32, 128), F32),
            pltpu.VMEM((8, 32, 128), F32),
            pltpu.VMEM((32, 128), F32),
            pltpu.VMEM((512, 128), F32),
            pltpu.VMEM((64, 512), BF16),
            pltpu.VMEM((64, 512), BF16),
            pltpu.VMEM((64, 512), F32),
            *[dma((1,))] * 9,
            dma((3,)),
            dma((4,)),
            dma(()),
            dma((6,)),
            dma((11,)),
            dma(()),
            pltpu.VMEM((2, 2, 512, 256), BF16),
            pltpu.VMEM((2, 512, 256), BF16),
        ],
        compiler_params=pltpu.CompilerParams(
            collective_id=0, has_side_effects=True, vmem_limit_bytes=40 * 1024 * 1024
        ),
        name="panel",
    )(*[pltpu.with_memory_space_constraint(x, pltpu.HBM) for x in (trail.reshape(8192, 128), *inputs)])
    trail_out, basis_out, coeff_out = pl.pallas_call(
        finish_kernel,
        out_shape=(jax.ShapeDtypeStruct((8192, 128), F32), small, small),
        in_specs=[VMEM] * 6,
        out_specs=(HBM,) * 3,
        scratch_shapes=[pltpu.VMEM((2, 64, 512), F32), dma((6,))],
        compiler_params=pltpu.CompilerParams(vmem_limit_bytes=40 * 1024 * 1024),
        name="finish",
    )(*results)
    return (trail_out.reshape(trail.shape), basis_out[:, None], coeff_out[:, None])


def solution(mesh):
    n_row = mesh.shape["row"]
    return jax.shard_map(
        functools.partial(body, n_row),
        mesh=mesh,
        in_specs=(
            P(None, "row", None, None, "col", None),
            P(None, "row", None, "col"),
            P(None, "row", None, "col"),
            P(None, "row", None, "col"),
            P(None, "col", None, "row"),
            P(None, "col", None, "row"),
            P(None, "col"),
            P(),
            P(),
            P(),
            P(),
            P(),
        ),
        out_specs=(
            P(None, "row", None, None, "col", None),
            P(None, "row", None, None),
            P(None, "row", None, None),
        ),
        check_vma=False,
    )
```
